32 devices in a mesh: gx: 8 (over y, x, core), gy: 4 (over z).
Axes of the slice: x: 2, y: 2, z: 4, core: 2. Of those that a mesh axis runs over, the one named last changes fastest.
Arguments:
- positions: float32 [3, 4096], P(None, ('gx', 'gy')), may hold values from 0 to 1
- species: int32 [4096], P(('gx', 'gy')), may hold values from 0 to 3
- neighbours: int32 [8, 4096], P(None, ('gx', 'gy')), may hold values from 0 to 639, as said below
- counts: int32 [4096], P(('gx', 'gy')), may hold values from 0 to 8, as said below
- live_atoms: int32 [32], P(('gx', 'gy')), may hold values from 64 to 128, as said below
- ghost_send: int32 [16384], P(('gx', 'gy')), may hold values from 0 to 127, as said below
- embed: float32 [128, 4], replicated, may hold values from -6 to 6
- site_energy: float32 [4], replicated, may hold values from -6 to 6
- radial_in: float32 [2, 64, 8], replicated, may hold values from -3 to 3
- radial_mid: float32 [2, 64, 64], replicated, may hold values from -1 to 1
- radial_out: float32 [2, 384, 64], replicated, may hold values from -1.5 to 1.5
- contract: float32 [2, 4, 6, 128], replicated, may hold values from -6 to 6
- mix: float32 [2, 128, 128], replicated, may hold values from -1 to 1
- skip: float32 [2, 128, 128], replicated, may hold values from -0.5 to 0.5
- read_one: float32 [128], replicated, may hold values from -1 to 1
- read_hidden: float32 [16, 128], replicated, may hold values from -1 to 1
- read_out: float32 [16], replicated, may hold values from -3 to 3
Outputs:
- energy: float32 [], replicated
- forces: float32 [3, 4096], P(None, ('gx', 'gy'))
- stress: float32 [3, 3], replicated
The draws below stay inside these ranges and needn't reach their ends.
Inputs may be any that keep to these rules, and one draw needn't show every extreme that they name: `live_atoms`: device 0 holds 128 real atoms. `counts`: zero for padding atoms; atom slot 0 of every device uses all 8 slots. `neighbours`: the used slots of an atom name a real atom of the same device (below its live count) or a ghost slot, numbered from 128 in the order of directions. `ghost_send`: each entry names a real atom of the sending device.
All inputs are finite; a program needn't handle non-finite values.
Results may differ from the reference program's by a relative error of at most 0.0003.
Values sent between devices are 32-bit elements; how exact they have to be, the bound alone decides.
A program may use at most 64 MiB of HBM per device.

```python
import jax
import jax.numpy as jnp
import numpy as np
from jax import lax

C = 128
H = 64
NB = 8
S = 4
RH = 16
K = 8
ATOM_DEV = 128
GHOST = 64
ATOMS = 4096
N_GX = 8
N_GY = 4


def live_table(key):
    device_total = ATOMS // ATOM_DEV
    table = jax.random.randint(jax.random.fold_in(key, 71), (device_total,), ATOM_DEV // 2, ATOM_DEV + 1)
    return table.at[0].set(ATOM_DEV)


def draw_live_atoms(key, part):
    return live_table(key)


def draw_counts(key, part):
    device_total = ATOMS // ATOM_DEV
    live = live_table(key)
    drawn = jax.random.randint(jax.random.fold_in(key, 72), (device_total, ATOM_DEV), K // 2, K + 1)
    drawn = jnp.where(jnp.arange(ATOM_DEV)[None, :] < live[:, None], drawn, 0)
    drawn = drawn.at[:, 0].set(K)
    return drawn.reshape(-1)


def draw_neighbours(key, part):
    device_total = ATOMS // ATOM_DEV
    live = live_table(key)
    limit = (live + 8 * GHOST)[None, :, None]
    drawn = jax.random.randint(jax.random.fold_in(key, 73), (K, device_total, ATOM_DEV), 0, limit)
    picked = jnp.where(drawn < live[None, :, None], drawn, drawn - live[None, :, None] + ATOM_DEV)
    return picked.reshape(K, -1)


def draw_ghost_send(key, part):
    device_total = ATOMS // ATOM_DEV
    live = live_table(key)
    drawn = jax.random.randint(jax.random.fold_in(key, 74), (device_total, 8 * GHOST), 0, live[:, None])
    return drawn.reshape(-1)


def set_ends(values, key, low, largest):
    longest = values.shape.index(max(values.shape))
    spots = []
    for shift in (0, 1):
        where = [jax.random.randint(jax.random.fold_in(key, axis), (), 0, length) for axis, length in enumerate(values.shape)]
        where[longest] = (where[longest] + shift) % values.shape[longest]
        spots.append(tuple(where))
    return values.at[spots[0]].set(low).at[spots[1]].set(largest)


def block_levels(stream_key, dims, pieces, smallest, high):
    def one(position, shards_of):
        steps = jax.random.uniform(jax.random.fold_in(jax.random.fold_in(stream_key, 6), position), (shards_of,), jnp.float32, smallest / len(pieces), high / len(pieces))
        return jnp.repeat(jnp.exp(steps), dims[position] // shards_of).reshape((-1,) + (1,) * (len(dims) - position - 1))

    loudness = one(*pieces[0])
    for cut in pieces[1:]:
        loudness = loudness * one(*cut)
    return loudness


def noise(key, extent, spread, most, held_as=jnp.bfloat16):
    values = jax.random.normal(key, extent, jnp.float32) * spread
    return jnp.minimum(jnp.maximum(values, -most), most).astype(held_as)


def setup_inputs(seed: int = 0) -> dict:
    splits = jax.random.split(jax.random.key(seed), 18)
    return {
        "positions": jnp.clip(1.0 * jax.random.uniform(splits[0], (3, ATOMS), jnp.float32) ** block_levels(splits[0], (3, ATOMS), ((1, 32),), -0.2, 0.2), 0.0, 1.0),
        "species": set_ends(jax.random.randint(splits[1], (ATOMS,), 0, S), jax.random.fold_in(splits[1], 1), 0, S - 1).astype(jnp.int32),
        "neighbours": draw_neighbours(jax.random.fold_in(splits[17], 71), 0),
        "counts": draw_counts(jax.random.fold_in(splits[17], 71), 0),
        "live_atoms": draw_live_atoms(jax.random.fold_in(splits[17], 71), 0),
        "ghost_send": draw_ghost_send(jax.random.fold_in(splits[17], 71), 0),
        "embed": noise(splits[6], (C, S), 1.0, 6.0, jnp.float32),
        "site_energy": noise(splits[7], (S,), 1.0, 6.0, jnp.float32),
        "radial_in": noise(splits[8], (2, H, NB), (NB // 2) ** -0.5, 3.0, jnp.float32),
        "radial_mid": noise(splits[9], (2, H, H), (H // 2) ** -0.5, 1.0, jnp.float32),
        "radial_out": noise(splits[10], (2, 3 * C, H), (H // 4) ** -0.5, 1.5, jnp.float32),
        "contract": noise(splits[11], (2, S, 6, C), 1.0, 6.0, jnp.float32),
        "mix": noise(splits[12], (2, C, C), (C // 4) ** -0.5, 1.0, jnp.float32),
        "skip": noise(splits[13], (2, C, C), C ** -0.5, 0.5, jnp.float32),
        "read_one": noise(splits[14], (C,), (C // 4) ** -0.5, 1.0, jnp.float32),
        "read_hidden": noise(splits[15], (RH, C), (C // 4) ** -0.5, 1.0, jnp.float32),
        "read_out": noise(splits[16], (RH,), (RH // 4) ** -0.5, 3.0, jnp.float32),
    }


highest = lax.Precision.HIGHEST
cut_sq = 4.0
span = 2.0
directions = ((-1, -1), (-1, 0), (-1, 1), (0, -1), (0, 1), (1, -1), (1, 0), (1, 1))

def edge_layer(edge_vec, valid, neigh_feat, self_feat, onehot, radial_in, radial_mid, radial_out, contract, mix, skip):
    slot_count, atom_count = valid.shape
    channels = mix.shape[0]
    basis_count = radial_in.shape[1]
    scaled = lax.optimization_barrier(jnp.sum(edge_vec * edge_vec, axis=0)) / cut_sq
    spacing = span / (basis_count - 1)
    centers = lax.iota(jnp.int32, basis_count).astype(jnp.float32) * spacing
    basis = jnp.exp(-0.5 * jnp.square((scaled[None] - centers[:, None, None]) / spacing))
    hidden = jax.nn.silu(jnp.dot(radial_in, basis.reshape(basis_count, slot_count * atom_count), precision=highest))
    hidden = jax.nn.silu(jnp.dot(radial_mid, hidden, precision=highest))
    radial = jnp.dot(radial_out, hidden, precision=highest).reshape(3, channels, slot_count, atom_count)
    radial = radial * (jnp.exp(-scaled) * valid)[None, None]
    weighted = radial * neigh_feat[None]
    comp_x, comp_y, comp_z = (edge_vec[0], edge_vec[1], edge_vec[2])
    harm_two = jnp.stack([comp_x * comp_y, comp_y * comp_z, comp_x * comp_z, 0.5 * (comp_x * comp_x - comp_y * comp_y), (2.0 * comp_z * comp_z - comp_x * comp_x - comp_y * comp_y) / 6.0])
    scalar_part = lax.optimization_barrier(jnp.sum(weighted[0], axis=1)) / slot_count
    vector_part = jnp.einsum('cka,mka->mca', weighted[1], edge_vec, precision=highest) / slot_count
    tensor_part = jnp.einsum('cka,mka->mca', weighted[2], harm_two, precision=highest) / slot_count
    square_one = lax.optimization_barrier(jnp.sum(vector_part * vector_part, axis=0))
    square_two = lax.optimization_barrier(jnp.sum(tensor_part * tensor_part, axis=0))
    tensor_xx = tensor_part[3] - tensor_part[4]
    tensor_yy = -tensor_part[3] - tensor_part[4]
    tensor_zz = 2.0 * tensor_part[4]
    triple = tensor_xx * vector_part[0] ** 2 + tensor_yy * vector_part[1] ** 2 + tensor_zz * vector_part[2] ** 2
    triple = triple + 2.0 * (tensor_part[0] * vector_part[0] * vector_part[1] + tensor_part[1] * vector_part[1] * vector_part[2] + tensor_part[2] * vector_part[0] * vector_part[2])
    paths = jnp.stack([scalar_part, scalar_part * scalar_part, square_one, square_two, scalar_part * square_one, triple])
    select = jnp.einsum('spc,sa->pca', contract, onehot, precision=highest)
    mixed = lax.optimization_barrier(jnp.sum(select * paths, axis=0))
    return jnp.dot(mix, mixed, precision=highest) + jnp.dot(skip, self_feat, precision=highest)

def local_setup(pos, kind, neigh, count, live, arrived, kinds):
    slot_count, atom_count = neigh.shape
    onehot_local = (kind[None, :] == lax.iota(jnp.int32, kinds)[:, None]).astype(jnp.float32)
    valid = (lax.iota(jnp.int32, slot_count)[:, None] < count[None, :]).astype(jnp.float32)
    live_mask = (lax.iota(jnp.int32, atom_count) < live).astype(jnp.float32)
    offsets = jnp.asarray(np.array([[heading[0] for heading in directions], [heading[1] for heading in directions], [0] * 8], np.float32))[:, :, None]
    ghost_pos = (arrived[0:3] + offsets).reshape(3, -1)
    ext_pos = jnp.concatenate([pos, ghost_pos], 1)
    edge_vec = ext_pos[:, neigh] - pos[:, None, :]
    ghost_kind = arrived[3].reshape(-1)
    onehot_ghost = (ghost_kind[None, :] == lax.iota(jnp.int32, kinds).astype(jnp.float32)[:, None]).astype(jnp.float32)
    onehot_ext = jnp.concatenate([onehot_local, onehot_ghost], 1)
    return (onehot_local, onehot_ext, valid, live_mask, edge_vec)

def layer_one(edge_vec, valid, onehot_local, onehot_ext, neigh, embed, weights):
    radial_in, radial_mid, radial_out, contract, mix, skip = weights
    start = jnp.dot(embed, onehot_ext, precision=highest)
    atom_count = valid.shape[1]
    return edge_layer(edge_vec, valid, start[:, neigh], start[:, :atom_count], onehot_local, radial_in[0], radial_mid[0], radial_out[0], contract[0], mix[0], skip[0])

def energy_two(edge_vec, neigh_feat, self_feat, valid, onehot_local, live_mask, weights, read_hidden, read_out):
    radial_in, radial_mid, radial_out, contract, mix, skip = weights
    second = edge_layer(edge_vec, valid, neigh_feat, self_feat, onehot_local, radial_in[1], radial_mid[1], radial_out[1], contract[1], mix[1], skip[1])
    site = jnp.dot(read_out, jax.nn.silu(jnp.dot(read_hidden, second, precision=highest)), precision=highest)
    return jnp.sum(site * live_mask)

def assemble(values, send):
    device_total, rows, atom_count = values.shape
    grid = values.reshape(N_GX, N_GY, rows, atom_count)
    send_grid = send.reshape(N_GX, N_GY, 8, GHOST)
    blocks = []
    for heading in range(8):
        shift_x, shift_y = directions[heading]
        source = jnp.roll(grid, (-shift_x, -shift_y), (0, 1))
        picks = jnp.roll(send_grid[:, :, heading], (-shift_x, -shift_y), (0, 1))
        blocks.append(jnp.take_along_axis(source, picks[:, :, None, :], axis=3))
    return jnp.stack(blocks, 3).reshape(device_total, rows, 8, GHOST)

def return_home(grads, send):
    device_total, rows = (grads.shape[0], grads.shape[1])
    grid = grads.reshape(N_GX, N_GY, rows, 8, GHOST)
    send_grid = send.reshape(N_GX, N_GY, 8, GHOST)
    total = jnp.zeros((device_total, rows, ATOM_DEV), jnp.float32)

    def place(block, picks):
        return jnp.zeros((rows, ATOM_DEV), jnp.float32).at[:, picks].add(block)
    for heading in range(8):
        shift_x, shift_y = directions[heading]
        moved = jnp.roll(grid[:, :, :, heading], (shift_x, shift_y), (0, 1)).reshape(device_total, rows, GHOST)
        picks = send_grid[:, :, heading].reshape(device_total, GHOST)
        total = total + jax.vmap(place)(moved, picks)
    return total

def reference(positions, species, neighbours, counts, live_atoms, ghost_send, embed, site_energy, radial_in, radial_mid, radial_out, contract, mix, skip, read_one, read_hidden, read_out):
    device_total = N_GX * N_GY
    weights = (radial_in, radial_mid, radial_out, contract, mix, skip)
    channels, kinds = embed.shape
    pos_dev = positions.reshape(3, device_total, ATOM_DEV).transpose(1, 0, 2)
    kind_dev = species.reshape(device_total, ATOM_DEV)
    neigh_dev = neighbours.reshape(K, device_total, ATOM_DEV).transpose(1, 0, 2)
    count_dev = counts.reshape(device_total, ATOM_DEV)
    send_dev = ghost_send.reshape(device_total, 8 * GHOST)
    packet_dev = jnp.concatenate([pos_dev, kind_dev[:, None, :].astype(jnp.float32)], 1)
    arrived_dev = assemble(packet_dev, send_dev)
    common = (pos_dev, kind_dev, neigh_dev, count_dev, live_atoms, arrived_dev)

    def first_pass(items):
        pos, kind, neigh, count, live, arrived = items
        onehot_local, onehot_ext, valid, live_mask, edge_vec = local_setup(pos, kind, neigh, count, live, arrived, kinds)
        return layer_one(edge_vec, valid, onehot_local, onehot_ext, neigh, embed, weights)
    first_dev = lax.map(first_pass, common)
    ghosts_dev = assemble(first_dev, send_dev)

    def second_pass(items):
        pos, kind, neigh, count, live, arrived, first, ghosts = items
        onehot_local, onehot_ext, valid, live_mask, edge_vec = local_setup(pos, kind, neigh, count, live, arrived, kinds)
        ext_first = jnp.concatenate([first, ghosts.reshape(channels, -1)], 1)

        def second(vec_in, neigh_in, self_in):
            return energy_two(vec_in, neigh_in, self_in, valid, onehot_local, live_mask, weights, read_hidden, read_out)
        energy_second, pullback = jax.vjp(second, edge_vec, ext_first[:, neigh], first)
        grad_vec, grad_neigh, grad_self = pullback(jnp.ones((), jnp.float32))
        ext_grad = jnp.zeros(ext_first.shape, jnp.float32).at[:, neigh].add(grad_neigh)
        atom_count = first.shape[1]
        own_grad = ext_grad[:, :atom_count] + grad_self + read_one[:, None] * live_mask[None, :]
        energy_first = jnp.sum(live_mask * (jnp.dot(read_one, first, precision=highest) + jnp.dot(site_energy, onehot_local, precision=highest)))
        return (energy_first + energy_second, grad_vec, own_grad, ext_grad[:, atom_count:].reshape(channels, 8, -1))
    energy_dev, grad_two_dev, own_dev, ghost_grad_dev = lax.map(second_pass, common + (first_dev, ghosts_dev))
    grad_first_dev = own_dev + return_home(ghost_grad_dev, send_dev)

    def third_pass(items):
        pos, kind, neigh, count, live, arrived, grad_first, grad_two = items
        onehot_local, onehot_ext, valid, live_mask, edge_vec = local_setup(pos, kind, neigh, count, live, arrived, kinds)

        def first_of(vec_in):
            return layer_one(vec_in, valid, onehot_local, onehot_ext, neigh, embed, weights)
        unused, pullback = jax.vjp(first_of, edge_vec)
        grad_vec = pullback(grad_first)[0] + grad_two
        atom_count = pos.shape[1]
        ext_pos_grad = jnp.zeros((3, onehot_ext.shape[1]), jnp.float32).at[:, neigh].add(grad_vec)
        own = ext_pos_grad[:, :atom_count] - lax.optimization_barrier(jnp.sum(grad_vec, axis=1))
        virial = jnp.einsum('ika,jka->ij', edge_vec, grad_vec, precision=highest)
        return (own, ext_pos_grad[:, atom_count:].reshape(3, 8, -1), virial)
    own_pos, ghost_pos_grad, virial_dev = lax.map(third_pass, common + (grad_first_dev, grad_two_dev))
    pos_grad = own_pos + return_home(ghost_pos_grad, send_dev)
    forces = -pos_grad.transpose(1, 0, 2).reshape(3, -1)
    live_total = jnp.sum(live_atoms).astype(jnp.float32)
    energy = jnp.sum(energy_dev) / live_total
    stress = lax.optimization_barrier(jnp.sum(virial_dev, axis=0)) / live_total
    return (energy, forces, stress)
```

```python
import functools

import jax
import jax.numpy as jnp
from jax import lax
from jax.experimental import pallas as pl
from jax.experimental.pallas import tpu as pltpu
from jax.sharding import PartitionSpec as P

f32 = jnp.float32
bf16 = jnp.bfloat16
MESH = pl.DeviceIdType.MESH
cut_sq = 4.0
span = 2.0
directions = ((-1, -1), (-1, 0), (-1, 1), (0, -1), (0, 1), (1, -1), (1, 0), (1, 1))
BLOCK = 16


def dot(a, b):
    return lax.dot_general(a, b, (((1,), (0,)), ((), ())), preferred_element_type=f32)


def dot_nt(a, b):
    return lax.dot_general(a, b, (((1,), (1,)), ((), ())), preferred_element_type=f32)


def halves(x):
    high = x.astype(bf16)
    return high, (x - high.astype(f32)).astype(bf16)


def stacked(x, parts):
    terms = []
    rest = x
    for _ in range(parts - 1):
        term = rest.astype(bf16).astype(f32)
        terms.append(term)
        rest = rest - term
    terms.append(rest)
    if (parts * x.shape[0]) % 16:
        terms.append(jnp.zeros_like(x))
    return jnp.concatenate(terms, 0).astype(bf16)


def unstacked(y, rows, parts):
    total = y[(parts - 1) * rows : parts * rows]
    for at in range(parts - 2, -1, -1):
        total = total + y[at * rows : (at + 1) * rows]
    return total


def dot3(a, b):
    a_high, a_low = halves(a)
    b_high, b_low = halves(b)
    return dot(a_high, b_high) + (dot(a_high, b_low) + dot(a_low, b_high))


def sub_iota(shape):
    return lax.broadcasted_iota(jnp.int32, shape, 0)


def lane_iota(shape):
    return lax.broadcasted_iota(jnp.int32, shape, 1)


def kernel(
    n_gx,
    n_gy,
    pos_ref,
    kind_ref,
    neigh_ref,
    count_ref,
    live_ref,
    send_ref,
    embed_ref,
    site_ref,
    win_ref,
    wmid_ref,
    wout_ref,
    contract_ref,
    mix_ref,
    skip_ref,
    one_ref,
    hidden_ref,
    out_ref,
    energy_ref,
    forces_ref,
    stress_ref,
    packet,
    table,
    embed_pad,
    place,
    place_back,
    pick,
    rows,
    grads,
    sel,
    rad0,
    drad0,
    rad1,
    drad1,
    feat0,
    feat1,
    deriv0,
    deriv1,
    mixed,
    first,
    gmix,
    gfeat,
    zed,
    gown,
    p_send,
    p_recv,
    f_send,
    f_recv,
    g_send,
    g_recv,
    q_send,
    q_recv,
    y_recv,
    x_send,
    x_recv,
    p_ss,
    p_rs,
    f_ss,
    f_rs,
    g_ss,
    g_rs,
    q_ss,
    q_rs,
    y_ss,
    y_rs,
    x_ss,
    x_rs,
):
    channels = embed_ref.shape[0]
    kinds = embed_ref.shape[1]
    slots, atoms = neigh_ref.shape
    edges = slots * atoms
    ghosts = send_ref.shape[1]
    ghost = ghosts // 8
    basis_count = win_ref.shape[2]
    hid = win_ref.shape[1]
    me_x = lax.axis_index("gx")
    me_y = lax.axis_index("gy")

    def at(off_x, off_y):
        return {
            "gx": lax.rem(me_x + (off_x + n_gx), n_gx),
            "gy": lax.rem(me_y + (off_y + n_gy), n_gy),
        }

    barrier = pltpu.get_barrier_semaphore()
    friends = [(ox, oy) for ox, oy in directions if ox and oy]
    friends += [(t, 0) for t in range(1, n_gx)] + [(0, t) for t in range(1, n_gy)]
    for ox, oy in friends:
        pl.semaphore_signal(barrier, inc=1, device_id=at(ox, oy), device_id_type=MESH)

    kind = kind_ref[...]
    packet[...] = jnp.zeros_like(packet)
    packet[0:3, :] = pos_ref[...]
    packet[3:4, :] = kind.astype(f32)
    own = packet[...]
    place_f = (sub_iota((atoms, ghosts)) == send_ref[...]).astype(f32)
    place[...] = place_f.astype(bf16)
    sent = unstacked(dot(stacked(own, 3), place[...]), 8, 3)
    for pair in range(4):
        p_send[pair] = sent[:, pair * 2 * ghost : (pair + 1) * 2 * ghost]

    def ghost_copy(src, dst, ss, rs, heading, sign):
        ox, oy = directions[heading]
        return pltpu.make_async_remote_copy(
            src_ref=src,
            dst_ref=dst,
            send_sem=ss.at[heading],
            recv_sem=rs.at[heading],
            device_id=at(sign * ox, sign * oy),
            device_id_type=MESH,
        )

    pl.semaphore_wait(barrier, len(friends))
    p_copies = [
        ghost_copy(p_send.at[d // 2], p_recv.at[d], p_ss, p_rs, d, -1) for d in range(8)
    ]
    for copy in p_copies:
        copy.start()

    for k in range(slots):
        pick[:, k * atoms : (k + 1) * atoms] = (
            (sub_iota((atoms + ghosts, atoms)) == neigh_ref[k : k + 1, :])
            .astype(f32)
            .astype(bf16)
        )
    for b in range(ghosts // atoms):
        place_back[b * atoms : (b + 1) * atoms, :] = jnp.transpose(
            place_f[:, b * atoms : (b + 1) * atoms]
        ).astype(bf16)
    table[...] = jnp.zeros_like(table)
    for layer in range(2):
        for s in range(kinds):
            base = (layer * kinds + s) * 8
            table[base : base + 6, :] = contract_ref[layer, s]
    table_high, table_low = halves(jnp.transpose(table[...]))
    for layer in range(2):
        for p in range(6):
            chosen = (
                (sub_iota((channels, atoms)) == kind * 8 + (layer * kinds * 8 + p))
                .astype(f32)
                .astype(bf16)
            )
            sel[layer, p] = dot(table_high, chosen) + dot(table_low, chosen)
    embed_pad[...] = jnp.zeros_like(embed_pad)
    embed_pad[:, 0:kinds] = embed_ref[...]
    embed_stack = stacked(embed_pad[...], 2)
    kind_local = (sub_iota((channels, atoms)) == kind).astype(f32).astype(bf16)
    start_self = unstacked(dot(embed_stack, kind_local), channels, 2)
    skip_part = dot3(skip_ref[0], start_self)
    read_mix = dot3(hidden_ref[...], mix_ref[1])
    read_skip = dot3(hidden_ref[...], skip_ref[1])
    live = (lane_iota((1, atoms)) < live_ref[0]).astype(f32)
    one_full = jnp.transpose(jnp.broadcast_to(one_ref[...], (atoms, channels)))
    readers = hidden_ref.shape[0]
    out_column = jnp.sum(
        jnp.where(
            sub_iota((readers, readers)) == lane_iota((readers, readers)), out_ref[...], 0.0
        ),
        axis=1,
        keepdims=True,
    )
    mix_back_high, mix_back_low = halves(jnp.transpose(mix_ref[0]))

    tiles = [own]
    lane = lane_iota((8, 2 * ghost))
    sub = sub_iota((8, 2 * ghost))
    for copy in p_copies:
        copy.wait_recv()
    for pair in range(4):
        (ax, ay), (bx, by) = directions[2 * pair], directions[2 * pair + 1]
        tile = jnp.where(lane < ghost, p_recv[2 * pair], p_recv[2 * pair + 1])
        off_x = jnp.where(lane < ghost, float(ax), float(bx))
        off_y = jnp.where(lane < ghost, float(ay), float(by))
        tiles.append(tile + jnp.where(sub == 0, off_x, jnp.where(sub == 1, off_y, 0.0)))
    ext = stacked(jnp.concatenate(tiles, 1), 3)
    rows[0:8, :] = unstacked(dot(ext, pick[...]), 8, 3)
    kind_edge = (
        (sub_iota((channels, edges)).astype(f32) == rows[3:4, :]).astype(f32).astype(bf16)
    )
    feat0[...] = unstacked(dot(embed_stack, kind_edge), channels, 2)
    for k in range(slots):
        lanes = slice(k * atoms, (k + 1) * atoms)
        x = rows[0:1, lanes] - pos_ref[0:1, :]
        y = rows[1:2, lanes] - pos_ref[1:2, :]
        z = rows[2:3, lanes] - pos_ref[2:3, :]
        rows[0:1, lanes] = x
        rows[1:2, lanes] = y
        rows[2:3, lanes] = z
        rows[3:4, lanes] = x * y
        rows[4:5, lanes] = y * z
        rows[5:6, lanes] = x * z
        rows[6:7, lanes] = 0.5 * (x * x - y * y)
        rows[7:8, lanes] = (2.0 * z * z - x * x - y * y) / 6.0
        squared = (x * x + y * y + z * z) / cut_sq
        rows[8:9, lanes] = squared
        valid = (count_ref[...] > k).astype(f32)
        rows[9:10, lanes] = jnp.exp(-squared) * valid * (1.0 / slots)

    spacing = span / (basis_count - 1)
    scaled = jnp.broadcast_to(rows[8:9, :], (basis_count, edges))
    gap = (scaled - sub_iota((basis_count, edges)).astype(f32) * spacing) / spacing
    basis = jnp.exp(-0.5 * gap * gap)
    basis_all = jnp.concatenate([basis, basis * gap * (-1.0 / spacing)], 1)

    def deep(w, x):
        w_high, w_low = halves(w)
        w_high, w_low = w_high.astype(f32), w_low.astype(f32)
        x_high = x.astype(bf16).astype(f32)
        left = jnp.concatenate([w_high, w_high, w_low], 1).astype(bf16)
        right = jnp.concatenate([x_high, x - x_high, x_high], 0).astype(bf16)
        return dot(left, right)

    def silu_pair(z):
        value, slope = z[:, :edges], z[:, edges:]
        gate = 1.0 / (1.0 + jnp.exp(-value))
        act = value * gate
        return act, (gate + act * (1.0 - gate)) * slope

    def network(layer):
        h, dh = silu_pair(deep(win_ref[layer], basis_all))
        h, dh = silu_pair(deep(wmid_ref[layer], jnp.concatenate([h, dh], 1)))
        env = rows[9:10, :]
        return h * env, (dh - h) * env

    def moments(layer, rad, feat, deriv):
        def step(block, carry):
            base = pl.multiple_of(block * BLOCK, BLOCK)
            here = pl.ds(base, BLOCK)
            acc = [jnp.zeros((BLOCK, atoms), f32) for _ in range(9)]
            for k in range(slots):
                lanes = slice(k * atoms, (k + 1) * atoms)
                h = feat[here, lanes]
                acc[0] = acc[0] + rad[pl.ds(base, BLOCK), lanes] * h
                w1 = rad[pl.ds(base + channels, BLOCK), lanes] * h
                w2 = rad[pl.ds(base + 2 * channels, BLOCK), lanes] * h
                for m in range(3):
                    acc[1 + m] = acc[1 + m] + w1 * rows[m : m + 1, lanes]
                for m in range(5):
                    acc[4 + m] = acc[4 + m] + w2 * rows[3 + m : 4 + m, lanes]
            a0, v0, v1, v2, xy, yz, xz, u, w = acc
            c0, c1, c2, c3, c4, c5 = [sel[layer, p, here, :] for p in range(6)]
            q1 = v0 * v0 + v1 * v1 + v2 * v2
            q2 = xy * xy + yz * yz + xz * xz + u * u + w * w
            m0 = (u - w) * v0 + xy * v1 + xz * v2
            m1 = xy * v0 - (u + w) * v1 + yz * v2
            m2 = xz * v0 + yz * v1 + 2.0 * w * v2
            triple = v0 * m0 + v1 * m1 + v2 * m2
            d1 = c2 + c4 * a0
            mixed[here, :] = (c0 + c1 * a0) * a0 + d1 * q1 + c3 * q2 + c5 * triple
            deriv[0, here, :] = c0 + 2.0 * c1 * a0 + c4 * q1
            deriv[1, here, :] = 2.0 * (d1 * v0 + c5 * m0)
            deriv[2, here, :] = 2.0 * (d1 * v1 + c5 * m1)
            deriv[3, here, :] = 2.0 * (d1 * v2 + c5 * m2)
            deriv[4, here, :] = 2.0 * (c3 * xy + c5 * (v0 * v1))
            deriv[5, here, :] = 2.0 * (c3 * yz + c5 * (v1 * v2))
            deriv[6, here, :] = 2.0 * (c3 * xz + c5 * (v0 * v2))
            deriv[7, here, :] = 2.0 * c3 * u + c5 * (v0 * v0 - v1 * v1)
            deriv[8, here, :] = 2.0 * c3 * w + c5 * (2.0 * v2 * v2 - v0 * v0 - v1 * v1)
            return carry

        lax.fori_loop(0, channels // BLOCK, step, 0)

    act0, slope0 = network(0)
    rad0[...] = deep(wout_ref[0], act0)
    moments(0, rad0, feat0, deriv0)
    first[...] = dot3(mix_ref[0], mixed[...]) + skip_part
    first_high, first_low = halves(first[...])
    sent_first = dot_nt(place_back[...], first_high) + dot_nt(place_back[...], first_low)
    for d in range(8):
        f_send[d] = sent_first[d * ghost : (d + 1) * ghost]
    f_copies = [ghost_copy(f_send.at[d], f_recv.at[d], f_ss, f_rs, d, -1) for d in range(8)]
    for copy in f_copies:
        copy.start()
    for copy in p_copies:
        copy.wait_send()

    act1, slope1 = network(1)
    rad1[...] = deep(wout_ref[1], act1)
    drad0[...] = deep(wout_ref[0], slope0)
    drad1[...] = deep(wout_ref[1], slope1)

    for copy in f_copies:
        copy.wait_recv()
    arrived = f_recv[...].reshape(ghosts, channels)
    turned = [first[...]] + [
        jnp.transpose(arrived[b * atoms : (b + 1) * atoms]) for b in range(ghosts // atoms)
    ]
    ext_first = stacked(jnp.concatenate(turned, 1), 2)
    feat1[...] = unstacked(dot(ext_first, pick[...]), channels, 2)
    moments(1, rad1, feat1, deriv1)
    inner = dot3(read_mix, mixed[...]) + dot3(read_skip, first[...])
    gate = 1.0 / (1.0 + jnp.exp(-inner))
    act = inner * gate
    g_inner = (gate + act * (1.0 - gate)) * out_column * live
    gmix[...] = dot3(jnp.transpose(read_mix), g_inner)

    def feature_grad(block, carry):
        base = pl.multiple_of(block * BLOCK, BLOCK)
        here = pl.ds(base, BLOCK)
        g = gmix[here, :]
        ga = [g * deriv1[m, here, :] for m in range(9)]
        for k in range(slots):
            lanes = slice(k * atoms, (k + 1) * atoms)
            t1 = sum(ga[1 + m] * rows[m : m + 1, lanes] for m in range(3))
            t2 = sum(ga[4 + m] * rows[3 + m : 4 + m, lanes] for m in range(5))
            total = ga[0] * rad1[pl.ds(base, BLOCK), lanes]
            total = total + t1 * rad1[pl.ds(base + channels, BLOCK), lanes]
            total = total + t2 * rad1[pl.ds(base + 2 * channels, BLOCK), lanes]
            high = total.astype(bf16)
            gfeat[pl.ds(base, BLOCK), lanes] = high
            gfeat[pl.ds(base + channels, BLOCK), lanes] = (total - high.astype(f32)).astype(bf16)
        return carry

    lax.fori_loop(0, channels // BLOCK, feature_grad, 0)
    back = dot_nt(pick[atoms : atoms + ghosts, :], gfeat[...])
    back = back[:, :channels] + back[:, channels:]
    for d in range(8):
        g_send[d] = back[d * ghost : (d + 1) * ghost]
    g_copies = [ghost_copy(g_send.at[d], g_recv.at[d], g_ss, g_rs, d, 1) for d in range(8)]
    for copy in g_copies:
        copy.start()
    for copy in f_copies:
        copy.wait_send()

    own_back = dot_nt(pick[0:atoms, :], gfeat[...])
    own_back = jnp.transpose(own_back[:, :channels] + own_back[:, channels:])
    gown[...] = own_back + dot3(jnp.transpose(read_skip), g_inner) + one_full * live
    energy_lanes = live * jnp.sum(one_full * first[...], axis=0, keepdims=True)
    energy_lanes = energy_lanes + live * jnp.sum(out_column * act, axis=0, keepdims=True)
    for s in range(kinds):
        energy_lanes = energy_lanes + jnp.where(kind == s, site_ref[s], 0.0) * live

    def edge_terms(rad, drad, feat, deriv, base, lanes):
        here = pl.ds(base, BLOCK)
        x, y, z = [rows[m : m + 1, lanes] for m in range(3)]
        h = feat[here, lanes]
        dv = [deriv[m, here, :] for m in range(9)]
        t1 = sum(dv[1 + m] * rows[m : m + 1, lanes] for m in range(3))
        t2 = sum(dv[4 + m] * rows[3 + m : 4 + m, lanes] for m in range(5))
        ds = dv[0] * drad[pl.ds(base, BLOCK), lanes]
        ds = ds + t1 * drad[pl.ds(base + channels, BLOCK), lanes]
        ds = ds + t2 * drad[pl.ds(base + 2 * channels, BLOCK), lanes]
        ds = ds * (2.0 / cut_sq)
        r1 = rad[pl.ds(base + channels, BLOCK), lanes]
        r2 = rad[pl.ds(base + 2 * channels, BLOCK), lanes]
        third = dv[8] * (1.0 / 3.0)
        gx = ds * x + r1 * dv[1] + r2 * (dv[4] * y + dv[6] * z + (dv[7] - third) * x)
        gy = ds * y + r1 * dv[2] + r2 * (dv[4] * x + dv[5] * z - (dv[7] + third) * y)
        gz = ds * z + r1 * dv[3] + r2 * (dv[5] * y + dv[6] * x + (2.0 * third) * z)
        return h * gx, h * gy, h * gz

    def first_terms(block, carry):
        base = pl.multiple_of(block * BLOCK, BLOCK)
        for k in range(slots):
            lanes = slice(k * atoms, (k + 1) * atoms)
            terms = edge_terms(rad0, drad0, feat0, deriv0, base, lanes)
            for i in range(3):
                zed[i, pl.ds(base, BLOCK), lanes] = terms[i]
        return carry

    lax.fori_loop(0, channels // BLOCK, first_terms, 0)
    for k in range(slots):
        lanes = slice(k * atoms, (k + 1) * atoms)

        def second_terms(block, carry):
            base = pl.multiple_of(block * BLOCK, BLOCK)
            terms = edge_terms(rad1, drad1, feat1, deriv1, base, lanes)
            g = gmix[pl.ds(base, BLOCK), :]
            return tuple(carry[i] + g * terms[i] for i in range(3))

        zero = jnp.zeros((BLOCK, atoms), f32)
        sums = lax.fori_loop(0, channels // BLOCK, second_terms, (zero, zero, zero))
        for i in range(3):
            grads[i : i + 1, lanes] = jnp.sum(sums[i], axis=0, keepdims=True)

    for copy in g_copies:
        copy.wait_recv()
    returned = g_recv[...].reshape(ghosts, channels)
    turned = jnp.concatenate(
        [jnp.transpose(returned[b * atoms : (b + 1) * atoms]) for b in range(ghosts // atoms)], 1
    )
    home = unstacked(dot(stacked(turned, 2), place_back[...]), channels, 2)
    g_high, g_low = halves(gown[...] + home)
    gmix[...] = (
        dot(mix_back_high, g_high) + dot(mix_back_high, g_low) + dot(mix_back_low, g_high)
    )
    for k in range(slots):
        lanes = slice(k * atoms, (k + 1) * atoms)
        for i in range(3):
            grads[i : i + 1, lanes] = grads[i : i + 1, lanes] + jnp.sum(
                gmix[...] * zed[i, :, lanes], axis=0, keepdims=True
            )
    for copy in g_copies:
        copy.wait_send()
    grads[3:8, :] = jnp.zeros((5, edges), f32)
    ext_grad = unstacked(dot_nt(stacked(grads[...], 2), pick[...]), 8, 2)
    for pair in range(4):
        q_send[pair] = ext_grad[:, atoms + pair * 2 * ghost : atoms + (pair + 1) * 2 * ghost]
    q_copies = [
        ghost_copy(q_send.at[d // 2], q_recv.at[d], q_ss, q_rs, d, 1) for d in range(8)
    ]
    for copy in q_copies:
        copy.start()

    partial = [energy_lanes, live]
    for a in range(3):
        for b in range(3):
            total = jnp.zeros((1, atoms), f32)
            for k in range(slots):
                lanes = slice(k * atoms, (k + 1) * atoms)
                total = total + rows[a : a + 1, lanes] * grads[b : b + 1, lanes]
            partial.append(total)
    partial.append(jnp.zeros((5, atoms), f32))
    y_recv[me_y] = jnp.concatenate(partial, 0)

    def line_copies(buf, ss, rs, me, count, where):
        outgoing = []
        incoming = []
        for t in range(1, count):
            source = lax.rem(me + (count - t), count)
            outgoing.append(
                pltpu.make_async_remote_copy(
                    src_ref=buf.at[me],
                    dst_ref=buf.at[me],
                    send_sem=ss.at[t],
                    recv_sem=rs.at[t],
                    device_id=where(t),
                    device_id_type=MESH,
                )
            )
            incoming.append(
                pltpu.make_async_remote_copy(
                    src_ref=buf.at[source],
                    dst_ref=buf.at[source],
                    send_sem=ss.at[t],
                    recv_sem=rs.at[t],
                    device_id=where(t),
                    device_id_type=MESH,
                )
            )
        return outgoing, incoming

    y_out, y_in = line_copies(y_recv, y_ss, y_rs, me_y, n_gy, lambda t: at(0, t))
    for copy in y_out:
        copy.start()
    own_grad = ext_grad[:, :atoms]
    for k in range(slots):
        own_grad = own_grad - grads[:, k * atoms : (k + 1) * atoms]
    for copy in y_in:
        copy.wait_recv()
    total = y_recv[0]
    for t in range(1, n_gy):
        total = total + y_recv[t]
    x_recv[me_x] = total
    x_out, x_in = line_copies(x_recv, x_ss, x_rs, me_x, n_gx, lambda t: at(t, 0))
    for copy in x_out:
        copy.start()

    for copy in q_copies:
        copy.wait_recv()
    tiles = [
        jnp.where(lane < ghost, q_recv[2 * pair], q_recv[2 * pair + 1]) for pair in range(4)
    ]
    home_pos = unstacked(dot(stacked(jnp.concatenate(tiles, 1), 2), place_back[...]), 8, 2)
    forces_ref[...] = -(own_grad + home_pos)[0:3]

    for copy in x_in:
        copy.wait_recv()
    total = x_recv[0]
    for t in range(1, n_gx):
        total = total + x_recv[t]
    total = jnp.sum(total, axis=1, keepdims=True)
    scaled_total = total / total[1:2]
    energy_ref[...] = scaled_total[0:1]
    corner_r, corner_c = sub_iota((3, 3)), lane_iota((3, 3))
    stress = jnp.zeros((3, 3), f32)
    for a in range(3):
        for b in range(3):
            value = scaled_total[2 + 3 * a + b : 3 + 3 * a + b]
            stress = jnp.where((corner_r == a) & (corner_c == b), value, stress)
    stress_ref[...] = stress
    for copy in q_copies + y_out + x_out:
        copy.wait_send()


def solution(mesh):
    n_gx, n_gy = mesh.shape["gx"], mesh.shape["gy"]

    def per_device(
        positions, species, neighbours, counts, live_atoms, ghost_send, embed, site_energy,
        radial_in, radial_mid, radial_out, contract, mix, skip, read_one, read_hidden, read_out,
    ):
        channels = embed.shape[0]
        slots, atoms = neighbours.shape
        edges = slots * atoms
        ghosts = ghost_send.shape[0]
        ghost = ghosts // 8
        vmem = pl.BlockSpec(memory_space=pltpu.VMEM)
        smem = pl.BlockSpec(memory_space=pltpu.SMEM)
        sems = pltpu.SemaphoreType.DMA
        wide = (channels, edges)
        scratch = [
            pltpu.VMEM((8, atoms), f32),
            pltpu.VMEM((channels, channels), f32),
            pltpu.VMEM((channels, channels), f32),
            pltpu.VMEM((atoms, ghosts), bf16),
            pltpu.VMEM((ghosts, atoms), bf16),
            pltpu.VMEM((atoms + ghosts, edges), bf16),
            pltpu.VMEM((16, edges), f32),
            pltpu.VMEM((8, edges), f32),
            pltpu.VMEM((2, 6, channels, atoms), f32),
            pltpu.VMEM((3 * channels, edges), f32),
            pltpu.VMEM((3 * channels, edges), f32),
            pltpu.VMEM((3 * channels, edges), f32),
            pltpu.VMEM((3 * channels, edges), f32),
            pltpu.VMEM(wide, f32),
            pltpu.VMEM(wide, f32),
            pltpu.VMEM((9, channels, atoms), f32),
            pltpu.VMEM((9, channels, atoms), f32),
            pltpu.VMEM((channels, atoms), f32),
            pltpu.VMEM((channels, atoms), f32),
            pltpu.VMEM((channels, atoms), f32),
            pltpu.VMEM((2 * channels, edges), bf16),
            pltpu.VMEM((3, channels, edges), f32),
            pltpu.VMEM((channels, atoms), f32),
            pltpu.VMEM((4, 8, 2 * ghost), f32),
            pltpu.VMEM((8, 8, 2 * ghost), f32),
            pltpu.VMEM((8, ghost, channels), f32),
            pltpu.VMEM((8, ghost, channels), f32),
            pltpu.VMEM((8, ghost, channels), f32),
            pltpu.VMEM((8, ghost, channels), f32),
            pltpu.VMEM((4, 8, 2 * ghost), f32),
            pltpu.VMEM((8, 8, 2 * ghost), f32),
            pltpu.VMEM((n_gy, 16, atoms), f32),
            pltpu.VMEM((16, atoms), f32),
            pltpu.VMEM((n_gx, 16, atoms), f32),
        ]
        scratch += [sems((8,))] * 8 + [sems((n_gy,))] * 2 + [sems((n_gx,))] * 2
        energy, forces, stress = pl.pallas_call(
            functools.partial(kernel, n_gx, n_gy),
            out_shape=(
                jax.ShapeDtypeStruct((1, 1), f32),
                jax.ShapeDtypeStruct((3, atoms), f32),
                jax.ShapeDtypeStruct((3, 3), f32),
            ),
            in_specs=[vmem] * 4 + [smem] + [vmem] * 2 + [smem] + [vmem] * 9,
            out_specs=(vmem, vmem, vmem),
            scratch_shapes=scratch,
            compiler_params=pltpu.CompilerParams(
                collective_id=0, has_side_effects=True, vmem_limit_bytes=50 * 1024 * 1024
            ),
        )(
            positions, species[None], neighbours, counts[None], live_atoms, ghost_send[None],
            embed, site_energy, radial_in, radial_mid, radial_out, contract, mix, skip,
            read_one[None], read_hidden, read_out[None],
        )
        return energy.reshape(()), forces, stress

    flat = P(("gx", "gy"))
    columns = P(None, ("gx", "gy"))
    return jax.shard_map(
        per_device,
        mesh=mesh,
        in_specs=(columns, flat, columns, flat, flat, flat) + (P(),) * 11,
        out_specs=(P(), columns, P()),
        check_vma=False,
    )
```

```python
import functools

import jax
import jax.numpy as jnp
from jax import lax
from jax.experimental import pallas as pl
from jax.experimental.pallas import tpu as pltpu
from jax.sharding import PartitionSpec as P

f32 = jnp.float32
bf16 = jnp.bfloat16
MESH = pl.DeviceIdType.MESH
cut_sq = 4.0
span = 2.0
directions = ((-1, -1), (-1, 0), (-1, 1), (0, -1), (0, 1), (1, -1), (1, 0), (1, 1))
BLOCK = 16


def dot(a, b):
    return lax.dot_general(a, b, (((1,), (0,)), ((), ())), preferred_element_type=f32)


def dot_nt(a, b):
    return lax.dot_general(a, b, (((1,), (1,)), ((), ())), preferred_element_type=f32)


def halves(x):
    high = x.astype(bf16)
    return high, (x - high.astype(f32)).astype(bf16)


def stacked(x, parts):
    terms = []
    rest = x
    for _ in range(parts - 1):
        term = rest.astype(bf16).astype(f32)
        terms.append(term)
        rest = rest - term
    terms.append(rest)
    if (parts * x.shape[0]) % 16:
        terms.append(jnp.zeros_like(x))
    return jnp.concatenate(terms, 0).astype(bf16)


def unstacked(y, rows, parts):
    total = y[(parts - 1) * rows : parts * rows]
    for at in range(parts - 2, -1, -1):
        total = total + y[at * rows : (at + 1) * rows]
    return total


def dot3(a, b):
    a_high, a_low = halves(a)
    b_high, b_low = halves(b)
    return dot(a_high, b_high) + (dot(a_high, b_low) + dot(a_low, b_high))


def terms3(x):
    high = x.astype(bf16).astype(f32)
    rest = x - high
    middle = rest.astype(bf16).astype(f32)
    return high, middle, rest - middle


def sixfold(w):
    high, middle, low = terms3(w)
    return jnp.concatenate([high, high, middle, high, middle, low], 1).astype(bf16)


def deep(left, x, full):
    high, middle, low = terms3(x)
    right = [high, middle, high]
    if full:
        right += [low, middle, high]
    right = jnp.concatenate(right, 0).astype(bf16)
    return dot(left[:, : right.shape[0]], right)


def sub_iota(shape):
    return lax.broadcasted_iota(jnp.int32, shape, 0)


def lane_iota(shape):
    return lax.broadcasted_iota(jnp.int32, shape, 1)


def kernel(
    n_gx,
    n_gy,
    *refs,
):
    ins = refs[:17]
    (energy_ref, forces_ref, stress_ref) = refs[17:20]
    (
        pos_ref,
        kind_ref,
        neigh_ref,
        count_ref,
        live_ref,
        send_ref,
        embed_ref,
        site_ref,
        win_ref,
        wmid_ref,
        wout_ref,
        contract_ref,
        mix_ref,
        skip_ref,
        one_ref,
        hidden_ref,
        out_ref,
    ) = refs[20:37]
    (
        packet,
        table,
        place,
        place_back,
        pick,
        rows,
        grads,
        sel,
        rad0,
        drad0,
        rad1,
        drad1,
        feat0,
        feat1,
        deriv0,
        deriv1,
        mixed,
        first,
        gmix,
        gfeat,
        zed,
        gown,
        p_send,
        p_recv,
        f_send,
        f_recv,
        g_send,
        g_recv,
        q_send,
        q_recv,
        mid6,
        out6,
        sums,
        p_ss,
        p_rs,
        f_ss,
        f_rs,
        g_ss,
        g_rs,
        q_ss,
        q_rs,
        s_ss,
        s_rs,
        in_sem,
    ) = refs[37:]
    kinds, channels = embed_ref.shape
    slots, atoms = neigh_ref.shape
    edges = slots * atoms
    ghosts = send_ref.shape[1]
    ghost = ghosts // 8
    basis_count, hid = win_ref.shape[1:]
    me_x = lax.axis_index("gx")
    me_y = lax.axis_index("gy")

    n_dev = n_gx * n_gy

    def wrapped(value, count):
        return jnp.where(value >= count, value - count, value)

    def at(off_x, off_y):
        return {
            "gx": wrapped(me_x + off_x % n_gx, n_gx),
            "gy": wrapped(me_y + off_y % n_gy, n_gy),
        }

    def peer(t, sign):
        off_x, off_y = t // n_gy, t % n_gy
        if sign < 0:
            off_x, off_y = n_gx - off_x, n_gy - off_y
        x, y = wrapped(me_x + off_x, n_gx), wrapped(me_y + off_y, n_gy)
        return {"gx": x, "gy": y}, x * n_gy + y

    def each_peer(act):
        if n_dev <= 64:
            for t in range(1, n_dev):
                act(t)
        else:
            lax.fori_loop(1, n_dev, lambda t, carry: (act(t), carry)[1], 0)

    barrier = pltpu.get_barrier_semaphore()

    def greet(t):
        pl.semaphore_signal(barrier, inc=1, device_id=peer(t, 1)[0], device_id_type=MESH)

    each_peer(greet)
    vmem_refs = refs[20:37]
    loads = [pltpu.make_async_copy(ins[i], vmem_refs[i], in_sem.at[i]) for i in range(17)]
    early = (0, 1, 5)
    for i in early + tuple(i for i in range(17) if i not in early):
        loads[i].start()
    for i in early:
        loads[i].wait()

    kind = kind_ref[...]
    packet[...] = jnp.zeros_like(packet)
    packet[0:3, :] = pos_ref[...]
    packet[3:4, :] = kind.astype(f32)
    own = packet[...]
    place_f = (sub_iota((atoms, ghosts)) == send_ref[...]).astype(f32)
    place[...] = place_f.astype(bf16)
    sent = unstacked(dot(stacked(own, 3), place[...]), 8, 3)
    for pair in range(4):
        p_send[pair] = sent[:, pair * 2 * ghost : (pair + 1) * 2 * ghost]

    def ghost_copy(src, dst, ss, rs, heading, sign):
        ox, oy = directions[heading]
        return pltpu.make_async_remote_copy(
            src_ref=src,
            dst_ref=dst,
            send_sem=ss.at[heading],
            recv_sem=rs.at[heading],
            device_id=at(sign * ox, sign * oy),
            device_id_type=MESH,
        )

    pl.semaphore_wait(barrier, n_dev - 1)
    p_copies = [
        ghost_copy(p_send.at[d // 2], p_recv.at[d], p_ss, p_rs, d, -1) for d in range(8)
    ]
    for copy in p_copies:
        copy.start()

    for i in range(17):
        if i not in early:
            loads[i].wait()
    for k in range(slots):
        pick[:, k * atoms : (k + 1) * atoms] = (
            (sub_iota((atoms + ghosts, atoms)) == neigh_ref[k : k + 1, :])
            .astype(f32)
            .astype(bf16)
        )
    for b in range(ghosts // atoms):
        place_back[b * atoms : (b + 1) * atoms, :] = jnp.transpose(
            place_f[:, b * atoms : (b + 1) * atoms]
        ).astype(bf16)
    table[...] = jnp.zeros_like(table)
    for layer in range(2):
        for p in range(6):
            base = (layer * 6 + p) * 8
            table[base : base + kinds, :] = contract_ref[layer, p]
        table[104 + 8 * layer : 112 + 8 * layer, 0:hid] = win_ref[layer]
    table[96 : 96 + kinds, :] = embed_ref[...]
    turned_table = jnp.transpose(table[...])
    table_terms = [term.astype(bf16) for term in terms3(turned_table)]
    win6 = [
        sixfold(turned_table[0:hid, 104 + 8 * l : 104 + 8 * l + basis_count]) for l in range(2)
    ]
    for layer in range(2):
        for p in range(6):
            chosen = (
                (sub_iota((channels, atoms)) == kind + (layer * 6 + p) * 8)
                .astype(f32)
                .astype(bf16)
            )
            sel[layer, p] = sum(dot(term, chosen) for term in table_terms)
        mid6[layer] = sixfold(wmid_ref[layer])
        for b in range(wout_ref.shape[2] // channels):
            part = slice(b * channels, (b + 1) * channels)
            out6[layer, part, :] = sixfold(jnp.transpose(wout_ref[layer, :, part]))
    embed_stack = stacked(turned_table, 3)
    kind_local = (sub_iota((channels, atoms)) == kind + 96).astype(f32).astype(bf16)
    start_self = unstacked(dot(embed_stack, kind_local), channels, 3)
    skip_part = deep(sixfold(skip_ref[0]), start_self, True)
    mix6 = sixfold(mix_ref[0])
    hidden6 = sixfold(hidden_ref[...])
    read_mix = deep(hidden6, mix_ref[1], True)
    read_skip = deep(hidden6, skip_ref[1], True)
    read_mix6, read_skip6 = sixfold(read_mix), sixfold(read_skip)
    live = (lane_iota((1, atoms)) < live_ref[0]).astype(f32)
    one_full = jnp.transpose(jnp.broadcast_to(one_ref[...], (atoms, channels)))
    readers = hidden_ref.shape[0]
    out_column = jnp.sum(
        jnp.where(
            sub_iota((readers, readers)) == lane_iota((readers, readers)), out_ref[...], 0.0
        ),
        axis=1,
        keepdims=True,
    )
    mix_back_high, mix_back_low = halves(jnp.transpose(mix_ref[0]))

    tiles = [own]
    lane = lane_iota((8, 2 * ghost))
    sub = sub_iota((8, 2 * ghost))
    for copy in p_copies:
        copy.wait_recv()
    for pair in range(4):
        (ax, ay), (bx, by) = directions[2 * pair], directions[2 * pair + 1]
        tile = jnp.where(lane < ghost, p_recv[2 * pair], p_recv[2 * pair + 1])
        off_x = jnp.where(lane < ghost, float(ax), float(bx))
        off_y = jnp.where(lane < ghost, float(ay), float(by))
        tiles.append(tile + jnp.where(sub == 0, off_x, jnp.where(sub == 1, off_y, 0.0)))
    ext = stacked(jnp.concatenate(tiles, 1), 3)
    rows[0:8, :] = unstacked(dot(ext, pick[...]), 8, 3)
    kind_edge = (
        ((sub_iota((channels, edges)) - 96).astype(f32) == rows[3:4, :]).astype(f32).astype(bf16)
    )
    feat0[...] = unstacked(dot(embed_stack, kind_edge), channels, 3)
    for k in range(slots):
        lanes = slice(k * atoms, (k + 1) * atoms)
        x = rows[0:1, lanes] - pos_ref[0:1, :]
        y = rows[1:2, lanes] - pos_ref[1:2, :]
        z = rows[2:3, lanes] - pos_ref[2:3, :]
        rows[0:1, lanes] = x
        rows[1:2, lanes] = y
        rows[2:3, lanes] = z
        rows[3:4, lanes] = x * y
        rows[4:5, lanes] = y * z
        rows[5:6, lanes] = x * z
        rows[6:7, lanes] = 0.5 * (x * x - y * y)
        rows[7:8, lanes] = (2.0 * z * z - x * x - y * y) / 6.0
        squared = (x * x + y * y + z * z) / cut_sq
        rows[8:9, lanes] = squared
        valid = (count_ref[...] > k).astype(f32)
        rows[9:10, lanes] = jnp.exp(-squared) * valid * (1.0 / slots)

    spacing = span / (basis_count - 1)
    scaled = jnp.broadcast_to(rows[8:9, :], (basis_count, edges))
    gap = (scaled - sub_iota((basis_count, edges)).astype(f32) * spacing) / spacing
    basis = jnp.exp(-0.5 * gap * gap)

    env = rows[9:10, :]

    def values(layer):
        act, gains = basis, []
        for left in (win6[layer], mid6[layer]):
            value = deep(left, act, True)
            gate = 1.0 / (1.0 + jnp.exp(-value))
            act = value * gate
            gains.append(gate + act * (1.0 - gate))
        act = act * env
        return act, gains

    def slopes(layer, act, gains):
        slope = gains[0] * deep(win6[layer], basis * gap * (-1.0 / spacing), False)
        slope = gains[1] * deep(mid6[layer], slope, False)
        return slope * env - act

    def moments(layer, rad, feat, deriv):
        def step(block, carry):
            base = pl.multiple_of(block * BLOCK, BLOCK)
            here = pl.ds(base, BLOCK)
            acc = [jnp.zeros((BLOCK, atoms), f32) for _ in range(9)]
            for k in range(slots):
                lanes = slice(k * atoms, (k + 1) * atoms)
                h = feat[here, lanes]
                acc[0] = acc[0] + rad[pl.ds(base, BLOCK), lanes] * h
                w1 = rad[pl.ds(base + channels, BLOCK), lanes] * h
                w2 = rad[pl.ds(base + 2 * channels, BLOCK), lanes] * h
                for m in range(3):
                    acc[1 + m] = acc[1 + m] + w1 * rows[m : m + 1, lanes]
                for m in range(5):
                    acc[4 + m] = acc[4 + m] + w2 * rows[3 + m : 4 + m, lanes]
            a0, v0, v1, v2, xy, yz, xz, u, w = acc
            c0, c1, c2, c3, c4, c5 = [sel[layer, p, here, :] for p in range(6)]
            q1 = v0 * v0 + v1 * v1 + v2 * v2
            q2 = xy * xy + yz * yz + xz * xz + u * u + w * w
            m0 = (u - w) * v0 + xy * v1 + xz * v2
            m1 = xy * v0 - (u + w) * v1 + yz * v2
            m2 = xz * v0 + yz * v1 + 2.0 * w * v2
            triple = v0 * m0 + v1 * m1 + v2 * m2
            d1 = c2 + c4 * a0
            mixed[here, :] = (c0 + c1 * a0) * a0 + d1 * q1 + c3 * q2 + c5 * triple
            deriv[0, here, :] = c0 + 2.0 * c1 * a0 + c4 * q1
            deriv[1, here, :] = 2.0 * (d1 * v0 + c5 * m0)
            deriv[2, here, :] = 2.0 * (d1 * v1 + c5 * m1)
            deriv[3, here, :] = 2.0 * (d1 * v2 + c5 * m2)
            deriv[4, here, :] = 2.0 * (c3 * xy + c5 * (v0 * v1))
            deriv[5, here, :] = 2.0 * (c3 * yz + c5 * (v1 * v2))
            deriv[6, here, :] = 2.0 * (c3 * xz + c5 * (v0 * v2))
            deriv[7, here, :] = 2.0 * c3 * u + c5 * (v0 * v0 - v1 * v1)
            deriv[8, here, :] = 2.0 * c3 * w + c5 * (2.0 * v2 * v2 - v0 * v0 - v1 * v1)
            return carry

        lax.fori_loop(0, channels // BLOCK, step, 0)

    act0, gains0 = values(0)
    rad0[...] = deep(out6[0], act0, True)
    moments(0, rad0, feat0, deriv0)
    first[...] = deep(mix6, mixed[...], True) + skip_part
    sent_first = sum(dot_nt(place_back[...], term.astype(bf16)) for term in terms3(first[...]))
    for d in range(8):
        f_send[d] = sent_first[d * ghost : (d + 1) * ghost]
    f_copies = [ghost_copy(f_send.at[d], f_recv.at[d], f_ss, f_rs, d, -1) for d in range(8)]
    for copy in f_copies:
        copy.start()
    for copy in p_copies:
        copy.wait_send()

    act1, gains1 = values(1)
    rad1[...] = deep(out6[1], act1, True)
    drad1[...] = deep(out6[1], slopes(1, act1, gains1), False)
    drad0[...] = deep(out6[0], slopes(0, act0, gains0), False)

    for copy in f_copies:
        copy.wait_recv()
    arrived = f_recv[...].reshape(ghosts, channels)
    turned = [first[...]] + [
        jnp.transpose(arrived[b * atoms : (b + 1) * atoms]) for b in range(ghosts // atoms)
    ]
    ext_first = stacked(jnp.concatenate(turned, 1), 3)
    feat1[...] = unstacked(dot(ext_first, pick[...]), channels, 3)
    moments(1, rad1, feat1, deriv1)
    inner = deep(read_mix6, mixed[...], True) + deep(read_skip6, first[...], True)
    gate = 1.0 / (1.0 + jnp.exp(-inner))
    act = inner * gate
    g_inner = (gate + act * (1.0 - gate)) * out_column * live
    gmix[...] = dot3(jnp.transpose(read_mix), g_inner)

    def feature_grad(block, carry):
        base = pl.multiple_of(block * BLOCK, BLOCK)
        here = pl.ds(base, BLOCK)
        g = gmix[here, :]
        ga = [g * deriv1[m, here, :] for m in range(9)]
        for k in range(slots):
            lanes = slice(k * atoms, (k + 1) * atoms)
            t1 = sum(ga[1 + m] * rows[m : m + 1, lanes] for m in range(3))
            t2 = sum(ga[4 + m] * rows[3 + m : 4 + m, lanes] for m in range(5))
            total = ga[0] * rad1[pl.ds(base, BLOCK), lanes]
            total = total + t1 * rad1[pl.ds(base + channels, BLOCK), lanes]
            total = total + t2 * rad1[pl.ds(base + 2 * channels, BLOCK), lanes]
            high = total.astype(bf16)
            gfeat[pl.ds(base, BLOCK), lanes] = high
            gfeat[pl.ds(base + channels, BLOCK), lanes] = (total - high.astype(f32)).astype(bf16)
        return carry

    lax.fori_loop(0, channels // BLOCK, feature_grad, 0)
    back = dot_nt(pick[atoms : atoms + ghosts, :], gfeat[...])
    back = back[:, :channels] + back[:, channels:]
    for d in range(8):
        g_send[d] = back[d * ghost : (d + 1) * ghost]
    g_copies = [ghost_copy(g_send.at[d], g_recv.at[d], g_ss, g_rs, d, 1) for d in range(8)]
    for copy in g_copies:
        copy.start()
    for copy in f_copies:
        copy.wait_send()

    own_back = dot_nt(pick[0:atoms, :], gfeat[...])
    own_back = jnp.transpose(own_back[:, :channels] + own_back[:, channels:])
    gown[...] = own_back + dot3(jnp.transpose(read_skip), g_inner) + one_full * live
    energy_lanes = live * jnp.sum(one_full * first[...], axis=0, keepdims=True)
    energy_lanes = energy_lanes + live * jnp.sum(out_column * act, axis=0, keepdims=True)
    for s in range(kinds):
        energy_lanes = energy_lanes + jnp.where(kind == s, site_ref[0:1, s : s + 1], 0.0) * live

    def edge_terms(rad, drad, feat, deriv, base, lanes):
        here = pl.ds(base, BLOCK)
        x, y, z = [rows[m : m + 1, lanes] for m in range(3)]
        h = feat[here, lanes]
        dv = [deriv[m, here, :] for m in range(9)]
        t1 = sum(dv[1 + m] * rows[m : m + 1, lanes] for m in range(3))
        t2 = sum(dv[4 + m] * rows[3 + m : 4 + m, lanes] for m in range(5))
        ds = dv[0] * drad[pl.ds(base, BLOCK), lanes]
        ds = ds + t1 * drad[pl.ds(base + channels, BLOCK), lanes]
        ds = ds + t2 * drad[pl.ds(base + 2 * channels, BLOCK), lanes]
        ds = ds * (2.0 / cut_sq)
        r1 = rad[pl.ds(base + channels, BLOCK), lanes]
        r2 = rad[pl.ds(base + 2 * channels, BLOCK), lanes]
        third = dv[8] * (1.0 / 3.0)
        gx = ds * x + r1 * dv[1] + r2 * (dv[4] * y + dv[6] * z + (dv[7] - third) * x)
        gy = ds * y + r1 * dv[2] + r2 * (dv[4] * x + dv[5] * z - (dv[7] + third) * y)
        gz = ds * z + r1 * dv[3] + r2 * (dv[5] * y + dv[6] * x + (2.0 * third) * z)
        return h * gx, h * gy, h * gz

    def first_terms(block, carry):
        base = pl.multiple_of(block * BLOCK, BLOCK)
        for k in range(slots):
            lanes = slice(k * atoms, (k + 1) * atoms)
            terms = edge_terms(rad0, drad0, feat0, deriv0, base, lanes)
            for i in range(3):
                zed[i, pl.ds(base, BLOCK), lanes] = terms[i]
        return carry

    lax.fori_loop(0, channels // BLOCK, first_terms, 0)
    for k in range(slots):
        lanes = slice(k * atoms, (k + 1) * atoms)

        def second_terms(block, carry):
            base = pl.multiple_of(block * BLOCK, BLOCK)
            terms = edge_terms(rad1, drad1, feat1, deriv1, base, lanes)
            g = gmix[pl.ds(base, BLOCK), :]
            return tuple(carry[i] + g * terms[i] for i in range(3))

        zero = jnp.zeros((BLOCK, atoms), f32)
        found = lax.fori_loop(0, channels // BLOCK, second_terms, (zero, zero, zero))
        for i in range(3):
            grads[i : i + 1, lanes] = jnp.sum(found[i], axis=0, keepdims=True)

    for copy in g_copies:
        copy.wait_recv()
    returned = g_recv[...].reshape(ghosts, channels)
    turned = jnp.concatenate(
        [jnp.transpose(returned[b * atoms : (b + 1) * atoms]) for b in range(ghosts // atoms)], 1
    )
    home = unstacked(dot(stacked(turned, 2), place_back[...]), channels, 2)
    g_high, g_low = halves(gown[...] + home)
    gmix[...] = (
        dot(mix_back_high, g_high) + dot(mix_back_high, g_low) + dot(mix_back_low, g_high)
    )
    for k in range(slots):
        lanes = slice(k * atoms, (k + 1) * atoms)
        for i in range(3):
            grads[i : i + 1, lanes] = grads[i : i + 1, lanes] + jnp.sum(
                gmix[...] * zed[i, :, lanes], axis=0, keepdims=True
            )
    for copy in g_copies:
        copy.wait_send()
    grads[3:8, :] = jnp.zeros((5, edges), f32)
    ext_grad = unstacked(dot_nt(stacked(grads[...], 2), pick[...]), 8, 2)
    for pair in range(4):
        q_send[pair] = ext_grad[:, atoms + pair * 2 * ghost : atoms + (pair + 1) * 2 * ghost]
    q_copies = [
        ghost_copy(q_send.at[d // 2], q_recv.at[d], q_ss, q_rs, d, 1) for d in range(8)
    ]
    for copy in q_copies:
        copy.start()

    partial = [energy_lanes, live]
    for a in range(3):
        for b in range(3):
            total = jnp.zeros((1, atoms), f32)
            for k in range(slots):
                lanes = slice(k * atoms, (k + 1) * atoms)
                total = total + rows[a : a + 1, lanes] * grads[b : b + 1, lanes]
            partial.append(total)
    partial.append(jnp.zeros((5, atoms), f32))
    column = jnp.sum(jnp.concatenate(partial, 0), axis=1, keepdims=True)
    mine = me_x * n_gy + me_y
    sums[mine] = jnp.sum(
        jnp.where(sub_iota((16, atoms)) == lane_iota((16, atoms)), column, 0.0),
        axis=0,
        keepdims=True,
    )

    def sum_copy(t, slot):
        return pltpu.make_async_remote_copy(
            src_ref=sums.at[slot],
            dst_ref=sums.at[slot],
            send_sem=s_ss.at[t],
            recv_sem=s_rs.at[t],
            device_id=peer(t, 1)[0],
            device_id_type=MESH,
        )

    each_peer(lambda t: sum_copy(t, mine).start())
    own_grad = ext_grad[:, :atoms]
    for k in range(slots):
        own_grad = own_grad - grads[:, k * atoms : (k + 1) * atoms]

    for copy in q_copies:
        copy.wait_recv()
    tiles = [
        jnp.where(lane < ghost, q_recv[2 * pair], q_recv[2 * pair + 1]) for pair in range(4)
    ]
    home_pos = unstacked(dot(stacked(jnp.concatenate(tiles, 1), 2), place_back[...]), 8, 2)
    forces_ref[...] = -(own_grad + home_pos)[0:3]

    each_peer(lambda t: sum_copy(t, peer(t, -1)[1]).wait_recv())
    total = jnp.sum(sums[...], axis=0)
    total = total / total[:, 1:2]
    energy_ref[...] = total[:, 0:1]
    for a in range(3):
        stress_ref[a : a + 1, :] = total[:, 2 + 3 * a : 5 + 3 * a]
    for copy in q_copies:
        copy.wait_send()
    each_peer(lambda t: sum_copy(t, mine).wait_send())


def solution(mesh):
    n_gx, n_gy = mesh.shape["gx"], mesh.shape["gy"]

    def per_device(
        positions, species, neighbours, counts, live_atoms, ghost_send, embed, site_energy,
        radial_in, radial_mid, radial_out, contract, mix, skip, read_one, read_hidden, read_out,
    ):
        channels, hid = embed.shape[0], radial_mid.shape[1]
        slots, atoms = neighbours.shape
        edges = slots * atoms
        ghosts = ghost_send.shape[0]
        ghost = ghosts // 8
        vmem = pl.BlockSpec(memory_space=pltpu.VMEM)
        sems = pltpu.SemaphoreType.DMA
        wide = (channels, edges)
        operands = (
            positions, species[None], neighbours, counts[None], live_atoms,
            ghost_send[None], embed.T, site_energy[None], jnp.swapaxes(radial_in, 1, 2),
            radial_mid, jnp.swapaxes(radial_out, 1, 2), jnp.swapaxes(contract, 1, 2),
            mix, skip, read_one[None], read_hidden, read_out[None],
        )
        scratch = [pltpu.VMEM(x.shape, x.dtype) for x in operands]
        scratch[4] = pltpu.SMEM(live_atoms.shape, live_atoms.dtype)
        scratch += [
            pltpu.VMEM((8, atoms), f32),
            pltpu.VMEM((channels, channels), f32),
            pltpu.VMEM((atoms, ghosts), bf16),
            pltpu.VMEM((ghosts, atoms), bf16),
            pltpu.VMEM((atoms + ghosts, edges), bf16),
            pltpu.VMEM((16, edges), f32),
            pltpu.VMEM((8, edges), f32),
            pltpu.VMEM((2, 6, channels, atoms), f32),
            pltpu.VMEM((3 * channels, edges), f32),
            pltpu.VMEM((3 * channels, edges), f32),
            pltpu.VMEM((3 * channels, edges), f32),
            pltpu.VMEM((3 * channels, edges), f32),
            pltpu.VMEM(wide, f32),
            pltpu.VMEM(wide, f32),
            pltpu.VMEM((9, channels, atoms), f32),
            pltpu.VMEM((9, channels, atoms), f32),
            pltpu.VMEM((channels, atoms), f32),
            pltpu.VMEM((channels, atoms), f32),
            pltpu.VMEM((channels, atoms), f32),
            pltpu.VMEM((2 * channels, edges), bf16),
            pltpu.VMEM((3, channels, edges), f32),
            pltpu.VMEM((channels, atoms), f32),
            pltpu.VMEM((4, 8, 2 * ghost), f32),
            pltpu.VMEM((8, 8, 2 * ghost), f32),
            pltpu.VMEM((8, ghost, channels), f32),
            pltpu.VMEM((8, ghost, channels), f32),
            pltpu.VMEM((8, ghost, channels), f32),
            pltpu.VMEM((8, ghost, channels), f32),
            pltpu.VMEM((4, 8, 2 * ghost), f32),
            pltpu.VMEM((8, 8, 2 * ghost), f32),
            pltpu.VMEM((2, hid, 6 * hid), bf16),
            pltpu.VMEM((2, 3 * channels, 6 * hid), bf16),
            pltpu.VMEM((n_gx * n_gy, 1, atoms), f32),
        ]
        scratch += [sems((8,))] * 8 + [sems((n_gx * n_gy,))] * 2 + [sems((17,))]
        energy, forces, stress = pl.pallas_call(
            functools.partial(kernel, n_gx, n_gy),
            out_shape=(
                jax.ShapeDtypeStruct((1, 1), f32),
                jax.ShapeDtypeStruct((3, atoms), f32),
                jax.ShapeDtypeStruct((3, 3), f32),
            ),
            in_specs=[pl.BlockSpec(memory_space=pltpu.HBM)] * 17,
            out_specs=(vmem, vmem, vmem),
            scratch_shapes=scratch,
            compiler_params=pltpu.CompilerParams(
                collective_id=0, has_side_effects=True, vmem_limit_bytes=67018752
            ),
        )(*operands)
        return energy.reshape(()), forces, stress

    flat = P(("gx", "gy"))
    columns = P(None, ("gx", "gy"))
    return jax.shard_map(
        per_device,
        mesh=mesh,
        in_specs=(columns, flat, columns, flat, flat, flat) + (P(),) * 11,
        out_specs=(P(), columns, P()),
        check_vma=False,
    )
```

```python
import functools

import jax
import jax.numpy as jnp
from jax import lax
from jax.experimental import pallas as pl
from jax.experimental.pallas import tpu as pltpu
from jax.sharding import PartitionSpec as P

f32 = jnp.float32
bf16 = jnp.bfloat16
MESH = pl.DeviceIdType.MESH
cut_sq = 4.0
span = 2.0
directions = ((-1, -1), (-1, 0), (-1, 1), (0, -1), (0, 1), (1, -1), (1, 0), (1, 1))
BLOCK = 16


def dot(a, b):
    return lax.dot_general(a, b, (((1,), (0,)), ((), ())), preferred_element_type=f32)


def dot_nt(a, b):
    return lax.dot_general(a, b, (((1,), (1,)), ((), ())), preferred_element_type=f32)


def halves(x):
    high = x.astype(bf16)
    return high, (x - high.astype(f32)).astype(bf16)


def stacked(x, parts):
    terms = []
    rest = x
    for _ in range(parts - 1):
        term = rest.astype(bf16).astype(f32)
        terms.append(term)
        rest = rest - term
    terms.append(rest)
    if (parts * x.shape[0]) % 16:
        terms.append(jnp.zeros_like(x))
    return jnp.concatenate(terms, 0).astype(bf16)


def unstacked(y, rows, parts):
    total = y[(parts - 1) * rows : parts * rows]
    for at in range(parts - 2, -1, -1):
        total = total + y[at * rows : (at + 1) * rows]
    return total


def dot3(a, b):
    a_high, a_low = halves(a)
    b_high, b_low = halves(b)
    return dot(a_high, b_high) + (dot(a_high, b_low) + dot(a_low, b_high))


def terms3(x):
    high = x.astype(bf16).astype(f32)
    rest = x - high
    middle = rest.astype(bf16).astype(f32)
    return high, middle, rest - middle


def sixfold(w):
    high, middle, low = terms3(w)
    return jnp.concatenate([high, high, middle, high, middle, low], 1).astype(bf16)


def deep(left, x, full):
    high, middle, low = terms3(x)
    right = [high, middle, high]
    if full:
        right += [low, middle, high]
    right = jnp.concatenate(right, 0).astype(bf16)
    return dot(left[:, : right.shape[0]], right)


def sub_iota(shape):
    return lax.broadcasted_iota(jnp.int32, shape, 0)


def lane_iota(shape):
    return lax.broadcasted_iota(jnp.int32, shape, 1)


def kernel(
    n_gx,
    n_gy,
    *refs,
):
    ins = refs[:17]
    (energy_ref, forces_ref, stress_ref) = refs[17:20]
    (
        pos_ref,
        kind_ref,
        neigh_ref,
        count_ref,
        live_ref,
        send_ref,
        embed_ref,
        site_ref,
        win_ref,
        wmid_ref,
        wout_ref,
        contract_ref,
        mix_ref,
        skip_ref,
        one_ref,
        hidden_ref,
        out_ref,
    ) = refs[20:37]
    (
        packet,
        table,
        place,
        place_back,
        pick,
        rows,
        grads,
        sel,
        rad0,
        drad0,
        rad1,
        drad1,
        feat0,
        feat1,
        deriv0,
        deriv1,
        mixed,
        first,
        gmix,
        gfeat,
        zed,
        gown,
        p_send,
        p_recv,
        f_send,
        f_recv,
        g_send,
        g_recv,
        q_send,
        q_recv,
        mid6,
        out6,
        sums,
        p_ss,
        p_rs,
        f_ss,
        f_rs,
        g_ss,
        g_rs,
        q_ss,
        q_rs,
        s_ss,
        s_rs,
        in_sem,
    ) = refs[37:]
    kinds, channels = embed_ref.shape
    slots, atoms = neigh_ref.shape
    edges = slots * atoms
    ghosts = send_ref.shape[1]
    ghost = ghosts // 8
    basis_count, hid = win_ref.shape[1:]
    me_x = lax.axis_index("gx")
    me_y = lax.axis_index("gy")

    n_dev = n_gx * n_gy

    def wrapped(value, count):
        return jnp.where(value >= count, value - count, value)

    def at(off_x, off_y):
        return {
            "gx": wrapped(me_x + off_x % n_gx, n_gx),
            "gy": wrapped(me_y + off_y % n_gy, n_gy),
        }

    def peer(t, sign):
        off_x, off_y = t // n_gy, t % n_gy
        if sign < 0:
            off_x, off_y = n_gx - off_x, n_gy - off_y
        x, y = wrapped(me_x + off_x, n_gx), wrapped(me_y + off_y, n_gy)
        return {"gx": x, "gy": y}, x * n_gy + y

    def each_peer(act):
        if n_dev <= 64:
            for t in range(1, n_dev):
                act(t)
        else:
            lax.fori_loop(1, n_dev, lambda t, carry: (act(t), carry)[1], 0)

    barrier = pltpu.get_barrier_semaphore()

    def greet(t):
        pl.semaphore_signal(barrier, inc=1, device_id=peer(t, 1)[0], device_id_type=MESH)

    each_peer(greet)
    vmem_refs = refs[20:37]
    loads = [pltpu.make_async_copy(ins[i], vmem_refs[i], in_sem.at[i]) for i in range(17)]
    early = (0, 1, 5)
    for i in early + tuple(i for i in range(17) if i not in early):
        loads[i].start()
    for i in early:
        loads[i].wait()

    kind = kind_ref[...]
    packet[...] = jnp.zeros_like(packet)
    packet[0:3, :] = pos_ref[...]
    packet[3:4, :] = kind.astype(f32)
    own = packet[...]
    place_f = (sub_iota((atoms, ghosts)) == send_ref[...]).astype(f32)
    place[...] = place_f.astype(bf16)
    sent = unstacked(dot(stacked(own, 3), place[...]), 8, 3)
    for pair in range(4):
        p_send[pair] = sent[:, pair * 2 * ghost : (pair + 1) * 2 * ghost]

    def ghost_copy(src, dst, ss, rs, heading, sign):
        ox, oy = directions[heading]
        return pltpu.make_async_remote_copy(
            src_ref=src,
            dst_ref=dst,
            send_sem=ss.at[heading],
            recv_sem=rs.at[heading],
            device_id=at(sign * ox, sign * oy),
            device_id_type=MESH,
        )

    pl.semaphore_wait(barrier, n_dev - 1)
    p_copies = [
        ghost_copy(p_send.at[d // 2], p_recv.at[d], p_ss, p_rs, d, -1) for d in range(8)
    ]
    for copy in p_copies:
        copy.start()

    for i in range(17):
        if i not in early:
            loads[i].wait()
    for k in range(slots):
        pick[:, k * atoms : (k + 1) * atoms] = (
            (sub_iota((atoms + ghosts, atoms)) == neigh_ref[k : k + 1, :])
            .astype(f32)
            .astype(bf16)
        )
    for b in range(ghosts // atoms):
        place_back[b * atoms : (b + 1) * atoms, :] = jnp.transpose(
            place_f[:, b * atoms : (b + 1) * atoms]
        ).astype(bf16)
    table[...] = jnp.zeros_like(table)
    for layer in range(2):
        for p in range(6):
            base = (layer * 6 + p) * 8
            table[base : base + kinds, :] = contract_ref[layer, p]
        table[104 + 8 * layer : 112 + 8 * layer, 0:hid] = win_ref[layer]
    table[96 : 96 + kinds, :] = embed_ref[...]
    turned_table = jnp.transpose(table[...])
    table_terms = [term.astype(bf16) for term in terms3(turned_table)]
    win6 = [
        sixfold(turned_table[0:hid, 104 + 8 * l : 104 + 8 * l + basis_count]) for l in range(2)
    ]
    for layer in range(2):
        for p in range(6):
            chosen = (
                (sub_iota((channels, atoms)) == kind + (layer * 6 + p) * 8)
                .astype(f32)
                .astype(bf16)
            )
            sel[layer, p] = sum(dot(term, chosen) for term in table_terms)
        mid6[layer] = sixfold(wmid_ref[layer])
        for b in range(wout_ref.shape[2] // channels):
            part = slice(b * channels, (b + 1) * channels)
            out6[layer, part, :] = sixfold(jnp.transpose(wout_ref[layer, :, part]))
    embed_stack = stacked(turned_table, 3)
    kind_local = (sub_iota((channels, atoms)) == kind + 96).astype(f32).astype(bf16)
    start_self = unstacked(dot(embed_stack, kind_local), channels, 3)
    skip_part = deep(sixfold(skip_ref[0]), start_self, True)
    mix6 = sixfold(mix_ref[0])
    hidden6 = sixfold(hidden_ref[...])
    read_mix = deep(hidden6, mix_ref[1], True)
    read_skip = deep(hidden6, skip_ref[1], True)
    read_mix6, read_skip6 = sixfold(read_mix), sixfold(read_skip)
    live = (lane_iota((1, atoms)) < live_ref[0]).astype(f32)
    one_full = jnp.transpose(jnp.broadcast_to(one_ref[...], (atoms, channels)))
    readers = hidden_ref.shape[0]
    out_column = jnp.sum(
        jnp.where(
            sub_iota((readers, readers)) == lane_iota((readers, readers)), out_ref[...], 0.0
        ),
        axis=1,
        keepdims=True,
    )
    mix_back_high, mix_back_low = halves(jnp.transpose(mix_ref[0]))

    tiles = [own]
    lane = lane_iota((8, 2 * ghost))
    sub = sub_iota((8, 2 * ghost))
    for copy in p_copies:
        copy.wait_recv()
    for pair in range(4):
        (ax, ay), (bx, by) = directions[2 * pair], directions[2 * pair + 1]
        tile = jnp.where(lane < ghost, p_recv[2 * pair], p_recv[2 * pair + 1])
        off_x = jnp.where(lane < ghost, float(ax), float(bx))
        off_y = jnp.where(lane < ghost, float(ay), float(by))
        tiles.append(tile + jnp.where(sub == 0, off_x, jnp.where(sub == 1, off_y, 0.0)))
    ext = stacked(jnp.concatenate(tiles, 1), 3)
    rows[0:8, :] = unstacked(dot(ext, pick[...]), 8, 3)
    kind_edge = (
        ((sub_iota((channels, edges)) - 96).astype(f32) == rows[3:4, :]).astype(f32).astype(bf16)
    )
    feat0[...] = unstacked(dot(embed_stack, kind_edge), channels, 3)
    for k in range(slots):
        lanes = slice(k * atoms, (k + 1) * atoms)
        x = rows[0:1, lanes] - pos_ref[0:1, :]
        y = rows[1:2, lanes] - pos_ref[1:2, :]
        z = rows[2:3, lanes] - pos_ref[2:3, :]
        rows[0:1, lanes] = x
        rows[1:2, lanes] = y
        rows[2:3, lanes] = z
        rows[3:4, lanes] = x * y
        rows[4:5, lanes] = y * z
        rows[5:6, lanes] = x * z
        rows[6:7, lanes] = 0.5 * (x * x - y * y)
        rows[7:8, lanes] = (2.0 * z * z - x * x - y * y) / 6.0
        squared = (x * x + y * y + z * z) / cut_sq
        rows[8:9, lanes] = squared
        valid = (count_ref[...] > k).astype(f32)
        rows[9:10, lanes] = jnp.exp(-squared) * valid * (1.0 / slots)

    spacing = span / (basis_count - 1)
    scaled = jnp.broadcast_to(rows[8:9, :], (basis_count, edges))
    gap = (scaled - sub_iota((basis_count, edges)).astype(f32) * spacing) / spacing
    basis = jnp.exp(-0.5 * gap * gap)

    env = rows[9:10, :]

    def values(layer):
        act, gains = basis, []
        for left in (win6[layer], mid6[layer]):
            value = deep(left, act, True)
            gate = 1.0 / (1.0 + jnp.exp(-value))
            act = value * gate
            gains.append(gate + act * (1.0 - gate))
        act = act * env
        return act, gains

    def slopes(layer, act, gains):
        slope = gains[0] * deep(win6[layer], basis * gap * (-1.0 / spacing), False)
        slope = gains[1] * deep(mid6[layer], slope, False)
        return slope * env - act

    def moments(layer, rad, feat, deriv):
        def step(block, carry):
            base = pl.multiple_of(block * BLOCK, BLOCK)
            here = pl.ds(base, BLOCK)
            acc = [jnp.zeros((BLOCK, atoms), f32) for _ in range(9)]
            for k in range(slots):
                lanes = slice(k * atoms, (k + 1) * atoms)
                h = feat[here, lanes]
                acc[0] = acc[0] + rad[pl.ds(base, BLOCK), lanes] * h
                w1 = rad[pl.ds(base + channels, BLOCK), lanes] * h
                w2 = rad[pl.ds(base + 2 * channels, BLOCK), lanes] * h
                for m in range(3):
                    acc[1 + m] = acc[1 + m] + w1 * rows[m : m + 1, lanes]
                for m in range(5):
                    acc[4 + m] = acc[4 + m] + w2 * rows[3 + m : 4 + m, lanes]
            a0, v0, v1, v2, xy, yz, xz, u, w = acc
            c0, c1, c2, c3, c4, c5 = [sel[layer, p, here, :] for p in range(6)]
            q1 = v0 * v0 + v1 * v1 + v2 * v2
            q2 = xy * xy + yz * yz + xz * xz + u * u + w * w
            m0 = (u - w) * v0 + xy * v1 + xz * v2
            m1 = xy * v0 - (u + w) * v1 + yz * v2
            m2 = xz * v0 + yz * v1 + 2.0 * w * v2
            triple = v0 * m0 + v1 * m1 + v2 * m2
            d1 = c2 + c4 * a0
            mixed[here, :] = (c0 + c1 * a0) * a0 + d1 * q1 + c3 * q2 + c5 * triple
            deriv[0, here, :] = c0 + 2.0 * c1 * a0 + c4 * q1
            deriv[1, here, :] = 2.0 * (d1 * v0 + c5 * m0)
            deriv[2, here, :] = 2.0 * (d1 * v1 + c5 * m1)
            deriv[3, here, :] = 2.0 * (d1 * v2 + c5 * m2)
            deriv[4, here, :] = 2.0 * (c3 * xy + c5 * (v0 * v1))
            deriv[5, here, :] = 2.0 * (c3 * yz + c5 * (v1 * v2))
            deriv[6, here, :] = 2.0 * (c3 * xz + c5 * (v0 * v2))
            deriv[7, here, :] = 2.0 * c3 * u + c5 * (v0 * v0 - v1 * v1)
            deriv[8, here, :] = 2.0 * c3 * w + c5 * (2.0 * v2 * v2 - v0 * v0 - v1 * v1)
            return carry

        lax.fori_loop(0, channels // BLOCK, step, 0)

    act0, gains0 = values(0)
    rad0[...] = deep(out6[0], act0, True)
    moments(0, rad0, feat0, deriv0)
    first[...] = deep(mix6, mixed[...], True) + skip_part
    sent_first = sum(dot_nt(place_back[...], term.astype(bf16)) for term in terms3(first[...]))
    for d in range(8):
        f_send[d] = sent_first[d * ghost : (d + 1) * ghost]
    f_copies = [ghost_copy(f_send.at[d], f_recv.at[d], f_ss, f_rs, d, -1) for d in range(8)]
    for copy in f_copies:
        copy.start()
    for copy in p_copies:
        copy.wait_send()

    act1, gains1 = values(1)
    rad1[...] = deep(out6[1], act1, True)
    drad1[...] = deep(out6[1], slopes(1, act1, gains1), False)
    drad0[...] = deep(out6[0], slopes(0, act0, gains0), False)

    def edge_terms(rad, drad, feat, deriv, base, lanes):
        here = pl.ds(base, BLOCK)
        x, y, z = [rows[m : m + 1, lanes] for m in range(3)]
        h = feat[here, lanes]
        dv = [deriv[m, here, :] for m in range(9)]
        t1 = sum(dv[1 + m] * rows[m : m + 1, lanes] for m in range(3))
        t2 = sum(dv[4 + m] * rows[3 + m : 4 + m, lanes] for m in range(5))
        ds = dv[0] * drad[pl.ds(base, BLOCK), lanes]
        ds = ds + t1 * drad[pl.ds(base + channels, BLOCK), lanes]
        ds = ds + t2 * drad[pl.ds(base + 2 * channels, BLOCK), lanes]
        ds = ds * (2.0 / cut_sq)
        r1 = rad[pl.ds(base + channels, BLOCK), lanes]
        r2 = rad[pl.ds(base + 2 * channels, BLOCK), lanes]
        third = dv[8] * (1.0 / 3.0)
        gx = ds * x + r1 * dv[1] + r2 * (dv[4] * y + dv[6] * z + (dv[7] - third) * x)
        gy = ds * y + r1 * dv[2] + r2 * (dv[4] * x + dv[5] * z - (dv[7] + third) * y)
        gz = ds * z + r1 * dv[3] + r2 * (dv[5] * y + dv[6] * x + (2.0 * third) * z)
        return h * gx, h * gy, h * gz

    def first_terms(block, carry):
        base = pl.multiple_of(block * BLOCK, BLOCK)
        for k in range(slots):
            lanes = slice(k * atoms, (k + 1) * atoms)
            terms = edge_terms(rad0, drad0, feat0, deriv0, base, lanes)
            for i in range(3):
                zed[i, pl.ds(base, BLOCK), lanes] = terms[i]
        return carry

    lax.fori_loop(0, channels // BLOCK, first_terms, 0)

    for copy in f_copies:
        copy.wait_recv()
    arrived = f_recv[...].reshape(ghosts, channels)
    turned = [first[...]] + [
        jnp.transpose(arrived[b * atoms : (b + 1) * atoms]) for b in range(ghosts // atoms)
    ]
    ext_first = stacked(jnp.concatenate(turned, 1), 3)
    feat1[...] = unstacked(dot(ext_first, pick[...]), channels, 3)
    moments(1, rad1, feat1, deriv1)
    inner = deep(read_mix6, mixed[...], True) + deep(read_skip6, first[...], True)
    gate = 1.0 / (1.0 + jnp.exp(-inner))
    act = inner * gate
    g_inner = (gate + act * (1.0 - gate)) * out_column * live
    gmix[...] = dot3(jnp.transpose(read_mix), g_inner)

    def feature_grad(block, carry):
        base = pl.multiple_of(block * BLOCK, BLOCK)
        here = pl.ds(base, BLOCK)
        g = gmix[here, :]
        ga = [g * deriv1[m, here, :] for m in range(9)]
        for k in range(slots):
            lanes = slice(k * atoms, (k + 1) * atoms)
            t1 = sum(ga[1 + m] * rows[m : m + 1, lanes] for m in range(3))
            t2 = sum(ga[4 + m] * rows[3 + m : 4 + m, lanes] for m in range(5))
            total = ga[0] * rad1[pl.ds(base, BLOCK), lanes]
            total = total + t1 * rad1[pl.ds(base + channels, BLOCK), lanes]
            total = total + t2 * rad1[pl.ds(base + 2 * channels, BLOCK), lanes]
            high = total.astype(bf16)
            gfeat[pl.ds(base, BLOCK), lanes] = high
            gfeat[pl.ds(base + channels, BLOCK), lanes] = (total - high.astype(f32)).astype(bf16)
        return carry

    lax.fori_loop(0, channels // BLOCK, feature_grad, 0)
    back = dot_nt(pick[atoms : atoms + ghosts, :], gfeat[...])
    back = back[:, :channels] + back[:, channels:]
    for d in range(8):
        g_send[d] = back[d * ghost : (d + 1) * ghost]
    g_copies = [ghost_copy(g_send.at[d], g_recv.at[d], g_ss, g_rs, d, 1) for d in range(8)]
    for copy in g_copies:
        copy.start()
    for copy in f_copies:
        copy.wait_send()

    own_back = dot_nt(pick[0:atoms, :], gfeat[...])
    own_back = jnp.transpose(own_back[:, :channels] + own_back[:, channels:])
    gown[...] = own_back + dot3(jnp.transpose(read_skip), g_inner) + one_full * live
    energy_lanes = live * jnp.sum(one_full * first[...], axis=0, keepdims=True)
    energy_lanes = energy_lanes + live * jnp.sum(out_column * act, axis=0, keepdims=True)
    for s in range(kinds):
        energy_lanes = energy_lanes + jnp.where(kind == s, site_ref[0:1, s : s + 1], 0.0) * live

    for k in range(slots):
        lanes = slice(k * atoms, (k + 1) * atoms)

        def second_terms(block, carry):
            base = pl.multiple_of(block * BLOCK, BLOCK)
            terms = edge_terms(rad1, drad1, feat1, deriv1, base, lanes)
            g = gmix[pl.ds(base, BLOCK), :]
            return tuple(carry[i] + g * terms[i] for i in range(3))

        zero = jnp.zeros((BLOCK, atoms), f32)
        found = lax.fori_loop(0, channels // BLOCK, second_terms, (zero, zero, zero))
        for i in range(3):
            grads[i : i + 1, lanes] = jnp.sum(found[i], axis=0, keepdims=True)

    for copy in g_copies:
        copy.wait_recv()
    returned = g_recv[...].reshape(ghosts, channels)
    turned = jnp.concatenate(
        [jnp.transpose(returned[b * atoms : (b + 1) * atoms]) for b in range(ghosts // atoms)], 1
    )
    home = unstacked(dot(stacked(turned, 2), place_back[...]), channels, 2)
    g_high, g_low = halves(gown[...] + home)
    gmix[...] = (
        dot(mix_back_high, g_high) + dot(mix_back_high, g_low) + dot(mix_back_low, g_high)
    )
    for k in range(slots):
        lanes = slice(k * atoms, (k + 1) * atoms)
        for i in range(3):
            grads[i : i + 1, lanes] = grads[i : i + 1, lanes] + jnp.sum(
                gmix[...] * zed[i, :, lanes], axis=0, keepdims=True
            )
    for copy in g_copies:
        copy.wait_send()
    grads[3:8, :] = jnp.zeros((5, edges), f32)
    ext_grad = unstacked(dot_nt(stacked(grads[...], 2), pick[...]), 8, 2)
    for pair in range(4):
        q_send[pair] = ext_grad[:, atoms + pair * 2 * ghost : atoms + (pair + 1) * 2 * ghost]
    q_copies = [
        ghost_copy(q_send.at[d // 2], q_recv.at[d], q_ss, q_rs, d, 1) for d in range(8)
    ]
    for copy in q_copies:
        copy.start()

    partial = [energy_lanes, live]
    for a in range(3):
        for b in range(3):
            total = jnp.zeros((1, atoms), f32)
            for k in range(slots):
                lanes = slice(k * atoms, (k + 1) * atoms)
                total = total + rows[a : a + 1, lanes] * grads[b : b + 1, lanes]
            partial.append(total)
    partial.append(jnp.zeros((5, atoms), f32))
    column = jnp.sum(jnp.concatenate(partial, 0), axis=1, keepdims=True)
    mine = me_x * n_gy + me_y
    sums[mine] = jnp.sum(
        jnp.where(sub_iota((16, atoms)) == lane_iota((16, atoms)), column, 0.0),
        axis=0,
        keepdims=True,
    )

    def sum_copy(t, slot):
        return pltpu.make_async_remote_copy(
            src_ref=sums.at[slot],
            dst_ref=sums.at[slot],
            send_sem=s_ss.at[t],
            recv_sem=s_rs.at[t],
            device_id=peer(t, 1)[0],
            device_id_type=MESH,
        )

    each_peer(lambda t: sum_copy(t, mine).start())
    own_grad = ext_grad[:, :atoms]
    for k in range(slots):
        own_grad = own_grad - grads[:, k * atoms : (k + 1) * atoms]

    for copy in q_copies:
        copy.wait_recv()
    tiles = [
        jnp.where(lane < ghost, q_recv[2 * pair], q_recv[2 * pair + 1]) for pair in range(4)
    ]
    home_pos = unstacked(dot(stacked(jnp.concatenate(tiles, 1), 2), place_back[...]), 8, 2)
    forces_ref[...] = -(own_grad + home_pos)[0:3]

    each_peer(lambda t: sum_copy(t, peer(t, -1)[1]).wait_recv())
    total = jnp.sum(sums[...], axis=0)
    total = total / total[:, 1:2]
    energy_ref[...] = total[:, 0:1]
    for a in range(3):
        stress_ref[a : a + 1, :] = total[:, 2 + 3 * a : 5 + 3 * a]
    for copy in q_copies:
        copy.wait_send()
    each_peer(lambda t: sum_copy(t, mine).wait_send())


def solution(mesh):
    n_gx, n_gy = mesh.shape["gx"], mesh.shape["gy"]

    def per_device(
        positions, species, neighbours, counts, live_atoms, ghost_send, embed, site_energy,
        radial_in, radial_mid, radial_out, contract, mix, skip, read_one, read_hidden, read_out,
    ):
        channels, hid = embed.shape[0], radial_mid.shape[1]
        slots, atoms = neighbours.shape
        edges = slots * atoms
        ghosts = ghost_send.shape[0]
        ghost = ghosts // 8
        vmem = pl.BlockSpec(memory_space=pltpu.VMEM)
        sems = pltpu.SemaphoreType.DMA
        wide = (channels, edges)
        operands = (
            positions, species[None], neighbours, counts[None], live_atoms,
            ghost_send[None], embed.T, site_energy[None], jnp.swapaxes(radial_in, 1, 2),
            radial_mid, jnp.swapaxes(radial_out, 1, 2), jnp.swapaxes(contract, 1, 2),
            mix, skip, read_one[None], read_hidden, read_out[None],
        )
        scratch = [pltpu.VMEM(x.shape, x.dtype) for x in operands]
        scratch[4] = pltpu.SMEM(live_atoms.shape, live_atoms.dtype)
        scratch += [
            pltpu.VMEM((8, atoms), f32),
            pltpu.VMEM((channels, channels), f32),
            pltpu.VMEM((atoms, ghosts), bf16),
            pltpu.VMEM((ghosts, atoms), bf16),
            pltpu.VMEM((atoms + ghosts, edges), bf16),
            pltpu.VMEM((16, edges), f32),
            pltpu.VMEM((8, edges), f32),
            pltpu.VMEM((2, 6, channels, atoms), f32),
            pltpu.VMEM((3 * channels, edges), f32),
            pltpu.VMEM((3 * channels, edges), f32),
            pltpu.VMEM((3 * channels, edges), f32),
            pltpu.VMEM((3 * channels, edges), f32),
            pltpu.VMEM(wide, f32),
            pltpu.VMEM(wide, f32),
            pltpu.VMEM((9, channels, atoms), f32),
            pltpu.VMEM((9, channels, atoms), f32),
            pltpu.VMEM((channels, atoms), f32),
            pltpu.VMEM((channels, atoms), f32),
            pltpu.VMEM((channels, atoms), f32),
            pltpu.VMEM((2 * channels, edges), bf16),
            pltpu.VMEM((3, channels, edges), f32),
            pltpu.VMEM((channels, atoms), f32),
            pltpu.VMEM((4, 8, 2 * ghost), f32),
            pltpu.VMEM((8, 8, 2 * ghost), f32),
            pltpu.VMEM((8, ghost, channels), f32),
            pltpu.VMEM((8, ghost, channels), f32),
            pltpu.VMEM((8, ghost, channels), f32),
            pltpu.VMEM((8, ghost, channels), f32),
            pltpu.VMEM((4, 8, 2 * ghost), f32),
            pltpu.VMEM((8, 8, 2 * ghost), f32),
            pltpu.VMEM((2, hid, 6 * hid), bf16),
            pltpu.VMEM((2, 3 * channels, 6 * hid), bf16),
            pltpu.VMEM((n_gx * n_gy, 1, atoms), f32),
        ]
        scratch += [sems((8,))] * 8 + [sems((n_gx * n_gy,))] * 2 + [sems((17,))]
        energy, forces, stress = pl.pallas_call(
            functools.partial(kernel, n_gx, n_gy),
            out_shape=(
                jax.ShapeDtypeStruct((1, 1), f32),
                jax.ShapeDtypeStruct((3, atoms), f32),
                jax.ShapeDtypeStruct((3, 3), f32),
            ),
            in_specs=[pl.BlockSpec(memory_space=pltpu.HBM)] * 17,
            out_specs=(vmem, vmem, vmem),
            scratch_shapes=scratch,
            compiler_params=pltpu.CompilerParams(
                collective_id=0, has_side_effects=True, vmem_limit_bytes=67018752
            ),
        )(*operands)
        return energy.reshape(()), forces, stress

    flat = P(("gx", "gy"))
    columns = P(None, ("gx", "gy"))
    return jax.shard_map(
        per_device,
        mesh=mesh,
        in_specs=(columns, flat, columns, flat, flat, flat) + (P(),) * 11,
        out_specs=(P(), columns, P()),
        check_vma=False,
    )
```
